32 devices in a mesh: bx: 4 (over y, x), by: 8 (over z, core).
Axes of the slice: x: 2, y: 2, z: 4, core: 2. Of those that a mesh axis runs over, the one named last changes fastest.
Arguments:
- forcing: float32 [1216, 1024], P('by', 'bx'), may hold values from -20 to 20
- guess: float32 [1216, 1024], P('by', 'bx'), may hold values from -3 to 3
- shift: float32 [1216, 1024], P('by', 'bx'), may hold values from 0.05 to 2
- ocean_mask: int32 [1216, 1024], P('by', 'bx'), may hold values 0 or 1
Outputs:
- solution_field: float32 [1216, 1024], P('by', 'bx')
- residual: float32 [1216, 1024], P('by', 'bx')
- residual_norm: float32 [], replicated
The draws below stay inside these ranges and needn't reach their ends.
All inputs are finite; a program needn't handle non-finite values. No bound on the sum of `ocean_mask` on one device may be relied on, other than what follows from the above.
Results may differ from the reference program's by a relative error of at most 0.00002.
Values sent between devices are 32-bit elements; how exact they have to be, the bound alone decides.
No kernel may reach another device: no remote copies, remote signals or barrier semaphores. Data moves between devices by JAX's collectives and lax.ppermute only.
A program may use at most 64 MiB of HBM per device.

```python
import math
import jax
import jax.numpy as jnp
from jax import lax

ITERS = 4
NX = 1024
NY = 1216


def draw_forcing(key, part):
    rows = jnp.arange(NY, dtype=jnp.float32)
    rising = 1.0 + 2.0 * rows / max(NY - 1, 1)
    rough = jnp.clip(jax.random.normal(key, (NY, NX), jnp.float32), -6.0, 6.0)
    values = rough * rising[:, None]
    return jnp.clip(values, -20.0, 20.0)


def touch_ends(entries, own_key, smallest, top_value):
    index_at = [jax.random.randint(jax.random.fold_in(own_key, axis), (), 0, length) for axis, length in enumerate(entries.shape)]
    widest = entries.shape.index(max(entries.shape))
    neighbour = index_at[:widest] + [(index_at[widest] + 1) % entries.shape[widest]] + index_at[widest + 1:]
    return entries.at[tuple(index_at)].set(smallest).at[tuple(neighbour)].set(top_value)


def levels(stream_key, dims, cuts, least, top_value):
    def one(axis_at, parts):
        draws = jax.random.uniform(jax.random.fold_in(jax.random.fold_in(stream_key, 6), axis_at), (parts,), jnp.float32, least / len(cuts), top_value / len(cuts))
        return jnp.repeat(jnp.exp(draws), dims[axis_at] // parts).reshape((-1,) + (1,) * (len(dims) - axis_at - 1))

    level = one(*cuts[0])
    for cut in cuts[1:]:
        level = level * one(*cut)
    return level


def scatter_about(key, shape, scale, reach, cuts=(), kind=jnp.bfloat16):
    entries = scale * jax.random.normal(key, shape, jnp.float32)
    if cuts:
        entries = entries * levels(key, shape, cuts, -0.22, 0.18)
    return jnp.clip(entries, -reach, reach).astype(kind)


def setup_inputs(seed: int = 0) -> dict:
    streams_of = jax.random.split(jax.random.key(seed), 5)
    return {
        "forcing": draw_forcing(jax.random.fold_in(streams_of[4], 71), 0),
        "guess": scatter_about(streams_of[1], (NY, NX), 0.5, 3.0, ((0, 8), (1, 4)), jnp.float32),
        "shift": jnp.clip(jnp.exp(math.log(2.0) - 3.6888794 * jax.random.uniform(streams_of[2], (NY, NX), jnp.float32) ** levels(streams_of[2], (NY, NX), ((0, 8), (1, 4)), -0.2, 0.2)), 0.05, 2.0),
        "ocean_mask": touch_ends((jax.random.randint(streams_of[3], (NY, NX), 0, 5) < 4).astype(jnp.int32), jax.random.fold_in(streams_of[3], 1), 0, 1),
    }


LOW_BOUND = 0.05
HIGH_BOUND = 14.5

def extend(values):
    zonal = jnp.concatenate([values[:, -1:], values, values[:, :1]], axis=1)
    top_row = zonal[-1, ::-1]
    bottom_row = jnp.zeros_like(top_row)
    return jnp.concatenate([bottom_row[None, :], zonal, top_row[None, :]], axis=0)

def nine_point(values, shift, mask_f):
    padded = extend(values)
    center = padded[1:-1, 1:-1]
    sides = padded[2:, 1:-1] + padded[:-2, 1:-1] + padded[1:-1, 2:] + padded[1:-1, :-2]
    corners = padded[2:, 2:] + padded[2:, :-2] + padded[:-2, 2:] + padded[:-2, :-2]
    return mask_f * ((6.0 + shift) * center - sides - 0.5 * corners)

def pair_add(first, second):
    total = first[0] + second[0]
    backed = total - first[0]
    error = first[0] - (total - backed) + (second[0] - backed)
    error = error + first[1] + second[1]
    upper = total + error
    lower = error - (upper - total)
    return (upper, lower)

def tree_total(uppers, lowers):
    while uppers.shape[0] > 1:
        if uppers.shape[0] % 2 == 1:
            uppers = jnp.concatenate([uppers, jnp.zeros((1,), uppers.dtype)])
            lowers = jnp.concatenate([lowers, jnp.zeros((1,), lowers.dtype)])
        uppers, lowers = pair_add((uppers[0::2], lowers[0::2]), (uppers[1::2], lowers[1::2]))
    return (uppers[0], lowers[0])

def reference(forcing, guess, shift, ocean_mask):
    mask_f = ocean_mask.astype(jnp.float32)
    theta = (HIGH_BOUND + LOW_BOUND) / 2.0
    delta = (HIGH_BOUND - LOW_BOUND) / 2.0
    sigma = theta / delta
    rho = 1.0 / sigma
    iterate = mask_f * guess
    resid = mask_f * forcing - nine_point(iterate, shift, mask_f)
    direction = resid / theta
    for sweep in range(ITERS):
        iterate = iterate + direction
        resid = resid - nine_point(direction, shift, mask_f)
        rho_next = 1.0 / (2.0 * sigma - rho)
        direction = rho_next * rho * direction + 2.0 * rho_next / delta * resid
        rho = rho_next
    row_sums = lax.optimization_barrier(jnp.sum(resid * resid, axis=1))
    upper, lower = tree_total(row_sums, jnp.zeros_like(row_sums))
    norm_value = jnp.sqrt((upper + lower) / (NX * NY))
    return (iterate, resid, norm_value)
```

```python
import functools

import jax
import jax.numpy as jnp
from jax import lax
from jax.experimental import pallas as pl
from jax.experimental.pallas import tpu as pltpu
from jax.sharding import PartitionSpec as P

ITERS = 4
LOW_BOUND = 0.05
HIGH_BOUND = 14.5

SUB = 8
LANE = 128
FIELDS = 3
VMEM = pl.BlockSpec(memory_space=pltpu.VMEM)
SMEM = pl.BlockSpec(memory_space=pltpu.SMEM)


def call(kernel, shapes, in_specs, out_specs, scratch=(), flops=100000):
    return pl.pallas_call(
        kernel,
        out_shape=shapes,
        in_specs=in_specs,
        out_specs=out_specs,
        scratch_shapes=scratch,
        cost_estimate=pl.CostEstimate(flops=flops, bytes_accessed=0, transcendentals=0),
    )


def masked_fields(forcing, guess, shift, ocean):
    zero = jnp.zeros_like(forcing)
    sea = ocean > 0
    return (
        jnp.where(sea, guess, zero),
        jnp.where(sea, forcing, zero),
        jnp.where(sea, 6.0 + shift, zero),
    )


def edge_kernel(odd_ref, *refs):
    low = [ref[...] for ref in refs[0:4]]
    top = [ref[...] for ref in refs[4:8]]
    near_ref, far_ref = refs[8:10]
    odd = odd_ref[0] == 1
    low = masked_fields(*low)
    top = masked_fields(*top)
    for f in range(FIELDS):
        rows = slice(f * SUB, (f + 1) * SUB)
        near_ref[rows, :] = jnp.where(odd, low[f], top[f])
        far_ref[rows, :] = jnp.where(odd, top[f], low[f])


def pack_columns(fields):
    rows, cols = fields[0].shape
    lane = lax.broadcasted_iota(jnp.int32, (rows, LANE), 1)
    packed = jnp.zeros((rows, LANE), jnp.float32)
    for f, field in enumerate(fields):
        at = f * SUB
        left = field[:, :LANE]
        left = pltpu.roll(left, at, 1) if at else left
        packed = jnp.where((lane >= at) & (lane < at + SUB), left, packed)
        at = (FIELDS + f) * SUB
        right = pltpu.roll(field[:, cols - LANE :], at + SUB, 1)
        packed = jnp.where((lane >= at) & (lane < at + SUB), right, packed)
    return packed


def block_kernel(forcing_ref, guess_ref, shift_ref, ocean_ref, x_ref, r_ref, c_ref, columns_ref):
    fields = masked_fields(forcing_ref[...], guess_ref[...], shift_ref[...], ocean_ref[...])
    for ref, field in zip((x_ref, r_ref, c_ref), fields):
        ref[...] = field
    packed = pack_columns(fields)
    width = columns_ref.shape[1]
    packed = jnp.concatenate([packed, jnp.zeros((width - packed.shape[0], LANE), jnp.float32)], axis=0)
    columns_ref[...] = packed.T[: 2 * FIELDS * SUB]


def mirrored(tile):
    back = LANE - 1 - lax.broadcasted_iota(jnp.int32, (SUB, LANE), 1)
    up = SUB - 1 - lax.broadcasted_iota(jnp.int32, (SUB, LANE), 0)
    parts = []
    for at in reversed(range(0, tile.shape[1], LANE)):
        part = jnp.take_along_axis(tile[:, at : at + LANE], back, axis=1)
        parts.append(jnp.take_along_axis(part, up, axis=0))
    return jnp.concatenate(parts, axis=1)


def halo_kernel(rows, where_ref, near_ref, far_ref, columns_ref, halo_ref, a_ref, b_ref):
    odd, fold, odd_x = where_ref[0] == 1, where_ref[1] == 1, where_ref[2] == 1
    n = FIELDS * SUB
    near, far = near_ref[...], far_ref[...]
    halo_ref[0:n, :] = jnp.where(odd, far, near)
    halo_ref[n : 2 * n, :] = jnp.where(odd, near, far)

    @pl.when(fold)
    def _():
        for f in range(FIELDS):
            at = slice(f * SUB, (f + 1) * SUB)
            halo_ref[at, :] = mirrored(halo_ref[at, :])

    fields = [
        jnp.concatenate([halo_ref[f * SUB : (f + 1) * SUB, :], halo_ref[n + f * SUB : n + (f + 1) * SUB, :]], axis=0)
        for f in range(FIELDS)
    ]
    packed = pack_columns(fields)
    width = columns_ref.shape[1]
    start = rows // LANE * LANE
    before, after = rows - start, width - rows - 2 * SUB
    pieces = [packed]
    if before:
        pieces.insert(0, jnp.zeros((before, LANE), jnp.float32))
    if after:
        pieces.append(jnp.zeros((after, LANE), jnp.float32))
    ends = jnp.concatenate(pieces, axis=0).T[: 2 * n]
    for at, first, second in ((slice(0, start), None, None), (slice(start, width), ends[:n], ends[n:])):
        if at.stop == at.start:
            continue
        left, right = columns_ref[0:n, at], columns_ref[n : 2 * n, at]
        if first is not None:
            left, right = left + first, right + second
        a_ref[:, at] = jnp.where(odd_x, left, right)
        b_ref[:, at] = jnp.where(odd_x, right, left)


def coefficients():
    theta = (HIGH_BOUND + LOW_BOUND) / 2.0
    delta = (HIGH_BOUND - LOW_BOUND) / 2.0
    sigma = theta / delta
    rho = 1.0 / sigma
    steps = []
    for _ in range(ITERS):
        following = 1.0 / (2.0 * sigma - rho)
        steps.append((following * rho, 2.0 * following / delta))
        rho = following
    return theta, steps


def pair_add(first, second):
    total = first[0] + second[0]
    backed = total - first[0]
    error = first[0] - (total - backed) + (second[0] - backed)
    error = error + first[1] + second[1]
    upper = total + error
    lower = error - (upper - total)
    return (upper, lower)


def pair_tree(pairs):
    while len(pairs) > 1:
        tail = pairs[len(pairs) // 2 * 2 :]
        pairs = [pair_add(pairs[i], pairs[i + 1]) for i in range(0, len(pairs) - 1, 2)] + tail
    return pairs[0]


def pair_total(pairs):
    total = pair_tree(pairs)
    for by in (4, 2, 1):
        total = pair_add(total, tuple(pltpu.roll(v, by, 0) for v in total))
    return total


def sweep_kernel(where_ref, x_ref, f_ref, c_ref, halo_ref, a_ref, b_ref, out_x_ref, out_r_ref, pair_ref, d_s, r_s, c_s):
    odd_x = where_ref[2] == 1
    rows, cols = x_ref.shape
    n = FIELDS * SUB
    tiles, inner = d_s.shape[0] // SUB, rows // SUB
    wide = cols + LANE
    high = d_s.shape[0]
    a, b = a_ref[...], b_ref[...]
    left, right = jnp.where(odd_x, a, b), jnp.where(odd_x, b, a)
    pieces = []
    for f in range(FIELDS):
        at = slice(f * SUB, (f + 1) * SUB)
        pieces += [left[at], right[at]]
    pieces.append(jnp.zeros((LANE - 2 * n, a.shape[1]), jnp.float32))
    sides = jnp.concatenate(pieces, axis=0).T
    for f, (ref, main) in enumerate(((d_s, x_ref), (r_s, f_ref), (c_s, c_ref))):
        at = slice(f * SUB, (f + 1) * SUB)
        ref[0:rows, 0:cols] = main[...]
        ref[rows : rows + SUB, 0:cols] = halo_ref[at, :]
        ref[rows + SUB : high, 0:cols] = halo_ref[n + f * SUB : n + (f + 1) * SUB, :]
        ref[:, cols:wide] = pltpu.roll(sides[0:high], LANE - (2 * f + 1) * SUB, 1)

    theta, steps = coefficients()
    row_id = lax.broadcasted_iota(jnp.int32, (SUB, wide), 0)
    first_row, last_row = row_id == 0, row_id == SUB - 1

    def across(i):
        v = d_s[i * SUB : (i + 1) * SUB, :]
        pair = pltpu.roll(v, 1, 1) + pltpu.roll(v, wide - 1, 1)
        mixed = v + 0.5 * pair
        return v, pair, pltpu.roll(mixed, 1, 0), pltpu.roll(mixed, SUB - 1, 0)

    squares = []
    for sweep in range(ITERS + 1):
        head, tail = across(0), across(tiles - 1)
        before, now = tail, head
        for i in range(tiles):
            if i < tiles - 2:
                after = across(i + 1)
            else:
                after = tail if i == tiles - 2 else head
            v, pair, down, up = now
            from_below = jnp.where(first_row, before[2], down)
            from_above = jnp.where(last_row, after[3], up)
            at = slice(i * SUB, (i + 1) * SUB)
            c = c_s[at, :]
            image = jnp.where(c > 0.0, c * v - (pair + (from_below + from_above)), jnp.zeros_like(c))
            r = r_s[at, :] - image
            if sweep < ITERS:
                r_s[at, :] = r
                if sweep == 0:
                    d = r * (1.0 / theta)
                else:
                    keep, gain = steps[sweep - 1]
                    d = keep * v + gain * r
                d_s[at, :] = d
                if i < inner:
                    old = x_ref[at, :] if sweep == 0 else out_x_ref[at, :]
                    out_x_ref[at, :] = old + d[:, :cols]
            elif i < inner:
                r = r[:, :cols]
                out_r_ref[at, :] = r
                squares.append(jnp.sum(r * r, axis=1, keepdims=True))
            before, now = now, after
    zero = jnp.zeros_like(squares[0])
    upper, lower = pair_total([(q, zero) for q in squares])
    lane = lax.broadcasted_iota(jnp.int32, (SUB, LANE), 1)
    tile = jnp.where(lane < LANE // 2, upper, lower)
    for i in range(pair_ref.shape[0] // SUB):
        pair_ref[i * SUB : (i + 1) * SUB, :] = tile


def norm_kernel(cells, pairs_ref, out_ref):
    pairs = []
    for i in range(pairs_ref.shape[0] // SUB):
        upper = pairs_ref[i * SUB : (i + 1) * SUB, :]
        pairs.append((upper, pltpu.roll(upper, LANE // 2, 1)))
    upper, lower = pair_total(pairs)
    out_ref[0] = jnp.sqrt((upper + lower) * (1.0 / cells))[0, 0]


def swap(value, mesh_shape, partner):
    wide, high = mesh_shape
    moves = []
    for b in range(wide):
        for j in range(high):
            other = partner(b, j)
            if other is not None:
                moves.append((b * high + j, other[0] * high + other[1]))
    return lax.ppermute(value, ("bx", "by"), moves)


def per_device(forcing, guess, shift, ocean):
    rows, cols = forcing.shape
    wide, high = lax.axis_size("bx"), lax.axis_size("by")
    devices = wide * high
    assert rows % SUB == 0 and cols % LANE == 0 and devices % SUB == 0
    assert wide % 2 == 0 and high % 2 == 0
    n = FIELDS * SUB
    tall = rows + 2 * SUB
    span = -(-tall // LANE) * LANE
    f32 = functools.partial(jax.ShapeDtypeStruct, dtype=jnp.float32)
    bx, by = lax.axis_index("bx"), lax.axis_index("by")
    where = jnp.stack([by % 2, (by == high - 1).astype(jnp.int32), bx % 2])

    last = rows // SUB - 1
    fields = (forcing, guess, shift, ocean)
    low_spec = pl.BlockSpec((SUB, cols), lambda i: (0, 0))
    top_spec = pl.BlockSpec((SUB, cols), lambda i: (last, 0))
    full_spec = pl.BlockSpec((n, cols), lambda i: (0, 0))
    near, far = pl.pallas_call(
        edge_kernel,
        grid=(1,),
        out_shape=(f32((n, cols)), f32((n, cols))),
        in_specs=[SMEM] + [low_spec] * 4 + [top_spec] * 4,
        out_specs=(full_spec, full_spec),
    )(where, *fields, *fields)

    def own_chip(b, j):
        return (b, j ^ 1)

    def next_chip(b, j):
        if j == 0:
            return None
        if j == high - 1:
            return (wide - 1 - b, j)
        return (b, ((j - 1) ^ 1) + 1)

    def even_pair(b, j):
        return (b ^ 1, j)

    def odd_pair(b, j):
        return ((((b - 1) % wide) ^ 1) + 1) % wide, j

    shape = (wide, high)
    near = swap(near, shape, own_chip)
    far = swap(far, shape, next_chip)
    x, f, c, columns = call(
        block_kernel,
        (f32((rows, cols)),) * 3 + (f32((2 * n, span)),),
        [VMEM] * 4,
        (VMEM,) * 4,
    )(*fields)
    halo, a, b = call(
        functools.partial(halo_kernel, rows),
        (f32((2 * n, cols)), f32((n, span)), f32((n, span))),
        [SMEM] + [VMEM] * 3,
        (VMEM,) * 3,
    )(where, near, far, columns)
    a = swap(a, shape, even_pair)
    b = swap(b, shape, odd_pair)
    x, r, pairs = call(
        sweep_kernel,
        (f32((rows, cols)), f32((rows, cols)), f32((devices, LANE))),
        [SMEM] + [VMEM] * 6,
        (VMEM,) * 3,
        [pltpu.VMEM((tall, cols + LANE), jnp.float32)] * 3,
    )(where, x, f, c, halo, a, b)
    pairs = lax.all_to_all(pairs, ("bx", "by"), 0, 0, tiled=True)
    cells = rows * cols * devices
    norm = call(functools.partial(norm_kernel, cells), f32((1,)), [VMEM], SMEM)(pairs)
    return (x, r, norm[0])


def solution(mesh):
    spec = P("by", "bx")
    return jax.shard_map(
        per_device, mesh=mesh, in_specs=(spec,) * 4, out_specs=(spec, spec, P()), check_vma=False
    )
```

```python
import functools

import jax
import jax.numpy as jnp
from jax import lax
from jax.experimental import pallas as pl
from jax.experimental.pallas import tpu as pltpu
from jax.sharding import PartitionSpec as P

ITERS = 4
LOW_BOUND = 0.05
HIGH_BOUND = 14.5

SUB = 8
LANE = 128
FIELDS = 3
VMEM = pl.BlockSpec(memory_space=pltpu.VMEM)
SMEM = pl.BlockSpec(memory_space=pltpu.SMEM)
HBM = pl.BlockSpec(memory_space=pltpu.HBM)
GRANT = pltpu.CompilerParams(vmem_limit_bytes=8 << 20)


def call(kernel, shapes, in_specs, out_specs, scratch=(), flops=100000):
    return pl.pallas_call(
        kernel,
        out_shape=shapes,
        in_specs=in_specs,
        out_specs=out_specs,
        scratch_shapes=scratch,
        cost_estimate=pl.CostEstimate(flops=flops, bytes_accessed=0, transcendentals=0),
        compiler_params=GRANT,
    )


def masked_fields(forcing, guess, shift, ocean):
    zero = jnp.zeros_like(forcing)
    sea = ocean > 0
    return (
        jnp.where(sea, guess, zero),
        jnp.where(sea, forcing, zero),
        jnp.where(sea, 6.0 + shift, zero),
    )


def is_odd(axis):
    return lax.rem(lax.axis_index(axis), 2) == 1


def edge_kernel(*refs):
    near_ref, far_ref = refs[4:6]
    low_s, top_s = refs[6:10], refs[10:14]
    sem = refs[14]
    rows = refs[0].shape[0]
    copies = []
    for i in range(4):
        copies.append(pltpu.make_async_copy(refs[i].at[0:SUB, :], low_s[i], sem.at[2 * i]))
        copies.append(pltpu.make_async_copy(refs[i].at[rows - SUB : rows, :], top_s[i], sem.at[2 * i + 1]))
    for copy in copies:
        copy.start()
    odd = is_odd("by")
    for copy in copies:
        copy.wait()
    low = masked_fields(*(ref[...] for ref in low_s))
    top = masked_fields(*(ref[...] for ref in top_s))
    for f in range(FIELDS):
        at = slice(f * SUB, (f + 1) * SUB)
        near_ref[at, :] = jnp.where(odd, low[f], top[f])
        far_ref[at, :] = jnp.where(odd, top[f], low[f])


def pack_columns(fields):
    rows, cols = fields[0].shape
    lane = lax.broadcasted_iota(jnp.int32, (rows, LANE), 1)
    packed = jnp.zeros((rows, LANE), jnp.float32)
    for f, field in enumerate(fields):
        at = f * SUB
        left = field[:, :LANE]
        left = pltpu.roll(left, at, 1) if at else left
        packed = jnp.where((lane >= at) & (lane < at + SUB), left, packed)
        at = (FIELDS + f) * SUB
        right = pltpu.roll(field[:, cols - LANE :], at + SUB, 1)
        packed = jnp.where((lane >= at) & (lane < at + SUB), right, packed)
    return packed


def block_kernel(*refs):
    x_ref, r_ref, c_ref, columns_ref = refs[4:8]
    held, sem = refs[8:12], refs[12]
    copies = [pltpu.make_async_copy(refs[i], held[i], sem.at[i]) for i in range(4)]
    for copy in copies:
        copy.start()
    for copy in copies:
        copy.wait()
    fields = masked_fields(*(ref[...] for ref in held))
    for ref, field in zip((x_ref, r_ref, c_ref), fields):
        ref[...] = field
    packed = pack_columns(fields)
    width = columns_ref.shape[1]
    packed = jnp.concatenate([packed, jnp.zeros((width - packed.shape[0], LANE), jnp.float32)], axis=0)
    columns_ref[...] = packed.T[: 2 * FIELDS * SUB]


def mirrored(tile):
    back = LANE - 1 - lax.broadcasted_iota(jnp.int32, (SUB, LANE), 1)
    up = SUB - 1 - lax.broadcasted_iota(jnp.int32, (SUB, LANE), 0)
    parts = []
    for at in reversed(range(0, tile.shape[1], LANE)):
        part = jnp.take_along_axis(tile[:, at : at + LANE], back, axis=1)
        parts.append(jnp.take_along_axis(part, up, axis=0))
    return jnp.concatenate(parts, axis=1)


def halo_kernel(rows, near_ref, far_ref, columns_ref, halo_ref, a_ref, b_ref):
    odd, odd_x = is_odd("by"), is_odd("bx")
    fold = lax.axis_index("by") == lax.axis_size("by") - 1
    n = FIELDS * SUB
    near, far = near_ref[...], far_ref[...]
    halo_ref[0:n, :] = jnp.where(odd, far, near)
    halo_ref[n : 2 * n, :] = jnp.where(odd, near, far)

    @pl.when(fold)
    def _():
        for f in range(FIELDS):
            at = slice(f * SUB, (f + 1) * SUB)
            halo_ref[at, :] = mirrored(halo_ref[at, :])

    fields = [
        jnp.concatenate([halo_ref[f * SUB : (f + 1) * SUB, :], halo_ref[n + f * SUB : n + (f + 1) * SUB, :]], axis=0)
        for f in range(FIELDS)
    ]
    packed = pack_columns(fields)
    width = columns_ref.shape[1]
    start = rows // LANE * LANE
    before, after = rows - start, width - rows - 2 * SUB
    pieces = [packed]
    if before:
        pieces.insert(0, jnp.zeros((before, LANE), jnp.float32))
    if after:
        pieces.append(jnp.zeros((after, LANE), jnp.float32))
    ends = jnp.concatenate(pieces, axis=0).T[: 2 * n]
    for at, first, second in ((slice(0, start), None, None), (slice(start, width), ends[:n], ends[n:])):
        if at.stop == at.start:
            continue
        left, right = columns_ref[0:n, at], columns_ref[n : 2 * n, at]
        if first is not None:
            left, right = left + first, right + second
        a_ref[:, at] = jnp.where(odd_x, left, right)
        b_ref[:, at] = jnp.where(odd_x, right, left)


def coefficients():
    theta = (HIGH_BOUND + LOW_BOUND) / 2.0
    delta = (HIGH_BOUND - LOW_BOUND) / 2.0
    sigma = theta / delta
    rho = 1.0 / sigma
    steps = []
    for _ in range(ITERS):
        following = 1.0 / (2.0 * sigma - rho)
        steps.append((following * rho, 2.0 * following / delta))
        rho = following
    return theta, steps


def pair_add(first, second):
    total = first[0] + second[0]
    backed = total - first[0]
    error = first[0] - (total - backed) + (second[0] - backed)
    error = error + first[1] + second[1]
    upper = total + error
    lower = error - (upper - total)
    return (upper, lower)


def pair_tree(pairs):
    while len(pairs) > 1:
        tail = pairs[len(pairs) // 2 * 2 :]
        pairs = [pair_add(pairs[i], pairs[i + 1]) for i in range(0, len(pairs) - 1, 2)] + tail
    return pairs[0]


def pair_total(pairs):
    total = pair_tree(pairs)
    for by in (4, 2, 1):
        total = pair_add(total, tuple(pltpu.roll(v, by, 0) for v in total))
    return total


def sweep_kernel(x_ref, f_ref, c_ref, halo_ref, a_ref, b_ref, out_x_ref, out_r_ref, pair_ref, d_s, r_s, c_s):
    odd_x = is_odd("bx")
    rows, cols = x_ref.shape
    n = FIELDS * SUB
    tiles, inner = d_s.shape[0] // SUB, rows // SUB
    wide = cols + LANE
    high = d_s.shape[0]
    a, b = a_ref[...], b_ref[...]
    left, right = jnp.where(odd_x, a, b), jnp.where(odd_x, b, a)
    pieces = []
    for f in range(FIELDS):
        at = slice(f * SUB, (f + 1) * SUB)
        pieces += [left[at], right[at]]
    pieces.append(jnp.zeros((LANE - 2 * n, a.shape[1]), jnp.float32))
    sides = jnp.concatenate(pieces, axis=0).T
    for f, (ref, main) in enumerate(((d_s, x_ref), (r_s, f_ref), (c_s, c_ref))):
        at = slice(f * SUB, (f + 1) * SUB)
        ref[0:rows, 0:cols] = main[...]
        ref[rows : rows + SUB, 0:cols] = halo_ref[at, :]
        ref[rows + SUB : high, 0:cols] = halo_ref[n + f * SUB : n + (f + 1) * SUB, :]
        ref[:, cols:wide] = pltpu.roll(sides[0:high], LANE - (2 * f + 1) * SUB, 1)

    theta, steps = coefficients()
    row_id = lax.broadcasted_iota(jnp.int32, (SUB, wide), 0)
    first_row, last_row = row_id == 0, row_id == SUB - 1

    def across(i):
        v = d_s[i * SUB : (i + 1) * SUB, :]
        pair = pltpu.roll(v, 1, 1) + pltpu.roll(v, wide - 1, 1)
        mixed = v + 0.5 * pair
        return v, pair, pltpu.roll(mixed, 1, 0), pltpu.roll(mixed, SUB - 1, 0)

    squares = []
    for sweep in range(ITERS + 1):
        head, tail = across(0), across(tiles - 1)
        before, now = tail, head
        for i in range(tiles):
            if i < tiles - 2:
                after = across(i + 1)
            else:
                after = tail if i == tiles - 2 else head
            v, pair, down, up = now
            from_below = jnp.where(first_row, before[2], down)
            from_above = jnp.where(last_row, after[3], up)
            at = slice(i * SUB, (i + 1) * SUB)
            c = c_s[at, :]
            image = jnp.where(c > 0.0, c * v - (pair + (from_below + from_above)), jnp.zeros_like(c))
            r = r_s[at, :] - image
            if sweep < ITERS:
                r_s[at, :] = r
                if sweep == 0:
                    d = r * (1.0 / theta)
                else:
                    keep, gain = steps[sweep - 1]
                    d = keep * v + gain * r
                d_s[at, :] = d
                if i < inner:
                    old = x_ref[at, :] if sweep == 0 else out_x_ref[at, :]
                    out_x_ref[at, :] = old + d[:, :cols]
            elif i < inner:
                r = r[:, :cols]
                out_r_ref[at, :] = r
                squares.append(jnp.sum(r * r, axis=1, keepdims=True))
            before, now = now, after
    zero = jnp.zeros_like(squares[0])
    upper, lower = pair_total([(q, zero) for q in squares])
    lane = lax.broadcasted_iota(jnp.int32, (SUB, LANE), 1)
    tile = jnp.where(lane < LANE // 2, upper, lower)
    for i in range(pair_ref.shape[0] // SUB):
        pair_ref[i * SUB : (i + 1) * SUB, :] = tile


def norm_kernel(cells, pairs_ref, out_ref):
    pairs = []
    for i in range(pairs_ref.shape[0] // SUB):
        upper = pairs_ref[i * SUB : (i + 1) * SUB, :]
        pairs.append((upper, pltpu.roll(upper, LANE // 2, 1)))
    upper, lower = pair_total(pairs)
    out_ref[0] = jnp.sqrt((upper + lower) * (1.0 / cells))[0, 0]


def swap(value, mesh_shape, partner):
    wide, high = mesh_shape
    moves = []
    for b in range(wide):
        for j in range(high):
            other = partner(b, j)
            if other is not None:
                moves.append((b * high + j, other[0] * high + other[1]))
    return lax.ppermute(value, ("bx", "by"), moves)


def per_device(forcing, guess, shift, ocean):
    rows, cols = forcing.shape
    wide, high = lax.axis_size("bx"), lax.axis_size("by")
    devices = wide * high
    assert rows % SUB == 0 and cols % LANE == 0 and devices % SUB == 0
    assert wide % 2 == 0 and high % 2 == 0
    n = FIELDS * SUB
    tall = rows + 2 * SUB
    span = -(-tall // LANE) * LANE
    f32 = functools.partial(jax.ShapeDtypeStruct, dtype=jnp.float32)
    fields = (forcing, guess, shift, ocean)
    edges = [pltpu.VMEM((SUB, cols), v.dtype) for v in fields]
    near, far = call(
        edge_kernel,
        (f32((n, cols)),) * 2,
        [HBM] * 4,
        (VMEM,) * 2,
        edges * 2 + [pltpu.SemaphoreType.DMA((8,))],
    )(*fields)

    def own_chip(b, j):
        return (b, j ^ 1)

    def next_chip(b, j):
        if j == 0:
            return None
        if j == high - 1:
            return (wide - 1 - b, j)
        return (b, ((j - 1) ^ 1) + 1)

    def even_pair(b, j):
        return (b ^ 1, j)

    def odd_pair(b, j):
        return ((((b - 1) % wide) ^ 1) + 1) % wide, j

    shape = (wide, high)
    near = swap(near, shape, own_chip)
    far = swap(far, shape, next_chip)
    x, f, c, columns = call(
        block_kernel,
        (f32((rows, cols)),) * 3 + (f32((2 * n, span)),),
        [HBM] * 4,
        (VMEM,) * 4,
        [pltpu.VMEM((rows, cols), v.dtype) for v in fields] + [pltpu.SemaphoreType.DMA((4,))],
    )(*fields)
    halo, a, b = call(
        functools.partial(halo_kernel, rows),
        (f32((2 * n, cols)), f32((n, span)), f32((n, span))),
        [VMEM] * 3,
        (VMEM,) * 3,
    )(near, far, columns)
    a = swap(a, shape, even_pair)
    b = swap(b, shape, odd_pair)
    x, r, pairs = call(
        sweep_kernel,
        (f32((rows, cols)), f32((rows, cols)), f32((devices, LANE))),
        [VMEM] * 6,
        (VMEM,) * 3,
        [pltpu.VMEM((tall, cols + LANE), jnp.float32)] * 3,
    )(x, f, c, halo, a, b)
    pairs = lax.all_to_all(pairs, ("bx", "by"), 0, 0, tiled=True)
    cells = rows * cols * devices
    norm = call(functools.partial(norm_kernel, cells), f32((1,)), [VMEM], SMEM)(pairs)
    return (x, r, norm[0])


def solution(mesh):
    spec = P("by", "bx")
    return jax.shard_map(
        per_device, mesh=mesh, in_specs=(spec,) * 4, out_specs=(spec, spec, P()), check_vma=False
    )
```

```python
import functools

import jax
import jax.numpy as jnp
from jax import lax
from jax.experimental import pallas as pl
from jax.experimental.pallas import tpu as pltpu
from jax.sharding import PartitionSpec as P

ITERS = 4
LOW_BOUND = 0.05
HIGH_BOUND = 14.5

SUB = 8
LANE = 128
FIELDS = 3
VMEM = pl.BlockSpec(memory_space=pltpu.VMEM)
SMEM = pl.BlockSpec(memory_space=pltpu.SMEM)
HBM = pl.BlockSpec(memory_space=pltpu.HBM)
GRANT = pltpu.CompilerParams(vmem_limit_bytes=8 << 20)


def call(kernel, shapes, in_specs, out_specs, scratch=(), flops=100000):
    return pl.pallas_call(
        kernel,
        out_shape=shapes,
        in_specs=in_specs,
        out_specs=out_specs,
        scratch_shapes=scratch,
        cost_estimate=pl.CostEstimate(flops=flops, bytes_accessed=0, transcendentals=0),
        compiler_params=GRANT,
    )


def masked_fields(forcing, guess, shift, ocean):
    zero = jnp.zeros_like(forcing)
    sea = ocean > 0
    return (
        jnp.where(sea, guess, zero),
        jnp.where(sea, forcing, zero),
        jnp.where(sea, 6.0 + shift, zero),
    )


def is_odd(axis):
    return lax.rem(lax.axis_index(axis), 2) == 1


def edge_kernel(*refs):
    near_ref, far_ref = refs[4:6]
    low_s, top_s = refs[6:10], refs[10:14]
    sem = refs[14]
    rows = refs[0].shape[0]
    copies = []
    for i in range(4):
        copies.append(pltpu.make_async_copy(refs[i].at[0:SUB, :], low_s[i], sem.at[2 * i]))
        copies.append(pltpu.make_async_copy(refs[i].at[rows - SUB : rows, :], top_s[i], sem.at[2 * i + 1]))
    for copy in copies:
        copy.start()
    odd = is_odd("by")
    for copy in copies:
        copy.wait()
    low = masked_fields(*(ref[...] for ref in low_s))
    top = masked_fields(*(ref[...] for ref in top_s))
    for f in range(FIELDS):
        at = slice(f * SUB, (f + 1) * SUB)
        near_ref[at, :] = jnp.where(odd, low[f], top[f])
        far_ref[at, :] = jnp.where(odd, top[f], low[f])


def pack_columns(fields):
    rows, cols = fields[0].shape
    lane = lax.broadcasted_iota(jnp.int32, (rows, LANE), 1)
    packed = jnp.zeros((rows, LANE), jnp.float32)
    for f, field in enumerate(fields):
        at = f * SUB
        left = field[:, :LANE]
        left = pltpu.roll(left, at, 1) if at else left
        packed = jnp.where((lane >= at) & (lane < at + SUB), left, packed)
        at = (FIELDS + f) * SUB
        right = pltpu.roll(field[:, cols - LANE :], at + SUB, 1)
        packed = jnp.where((lane >= at) & (lane < at + SUB), right, packed)
    return packed


def block_kernel(*refs):
    x_ref, r_ref, c_ref, columns_ref = refs[4:8]
    held, sem = refs[8:12], refs[12]
    copies = [pltpu.make_async_copy(refs[i], held[i], sem.at[i]) for i in range(4)]
    for copy in copies:
        copy.start()
    for copy in copies:
        copy.wait()
    fields = masked_fields(*(ref[...] for ref in held))
    for ref, field in zip((x_ref, r_ref, c_ref), fields):
        ref[...] = field
    packed = pack_columns(fields)
    width = columns_ref.shape[1]
    packed = jnp.concatenate([packed, jnp.zeros((width - packed.shape[0], LANE), jnp.float32)], axis=0)
    columns_ref[...] = packed.T[: 2 * FIELDS * SUB]


def mirrored(tile):
    back = LANE - 1 - lax.broadcasted_iota(jnp.int32, (SUB, LANE), 1)
    up = SUB - 1 - lax.broadcasted_iota(jnp.int32, (SUB, LANE), 0)
    parts = []
    for at in reversed(range(0, tile.shape[1], LANE)):
        part = jnp.take_along_axis(tile[:, at : at + LANE], back, axis=1)
        parts.append(jnp.take_along_axis(part, up, axis=0))
    return jnp.concatenate(parts, axis=1)


def halo_kernel(rows, near_ref, far_ref, columns_ref, halo_ref, a_ref, b_ref):
    odd, odd_x = is_odd("by"), is_odd("bx")
    fold = lax.axis_index("by") == lax.axis_size("by") - 1
    n = FIELDS * SUB
    near, far = near_ref[...], far_ref[...]
    halo_ref[0:n, :] = jnp.where(odd, far, near)
    halo_ref[n : 2 * n, :] = jnp.where(odd, near, far)

    @pl.when(fold)
    def _():
        for f in range(FIELDS):
            at = slice(f * SUB, (f + 1) * SUB)
            halo_ref[at, :] = mirrored(halo_ref[at, :])

    fields = [
        jnp.concatenate([halo_ref[f * SUB : (f + 1) * SUB, :], halo_ref[n + f * SUB : n + (f + 1) * SUB, :]], axis=0)
        for f in range(FIELDS)
    ]
    packed = pack_columns(fields)
    width = columns_ref.shape[1]
    start = rows // LANE * LANE
    before, after = rows - start, width - rows - 2 * SUB
    pieces = [packed]
    if before:
        pieces.insert(0, jnp.zeros((before, LANE), jnp.float32))
    if after:
        pieces.append(jnp.zeros((after, LANE), jnp.float32))
    ends = jnp.concatenate(pieces, axis=0).T[: 2 * n]
    for at, first, second in ((slice(0, start), None, None), (slice(start, width), ends[:n], ends[n:])):
        if at.stop == at.start:
            continue
        left, right = columns_ref[0:n, at], columns_ref[n : 2 * n, at]
        if first is not None:
            left, right = left + first, right + second
        a_ref[:, at] = jnp.where(odd_x, left, right)
        b_ref[:, at] = jnp.where(odd_x, right, left)


def coefficients():
    theta = (HIGH_BOUND + LOW_BOUND) / 2.0
    delta = (HIGH_BOUND - LOW_BOUND) / 2.0
    sigma = theta / delta
    rho = 1.0 / sigma
    steps = []
    for _ in range(ITERS):
        following = 1.0 / (2.0 * sigma - rho)
        steps.append((following * rho, 2.0 * following / delta))
        rho = following
    return theta, steps


def pair_add(first, second):
    total = first[0] + second[0]
    backed = total - first[0]
    error = first[0] - (total - backed) + (second[0] - backed)
    error = error + first[1] + second[1]
    upper = total + error
    lower = error - (upper - total)
    return (upper, lower)


def pair_tree(pairs):
    while len(pairs) > 1:
        tail = pairs[len(pairs) // 2 * 2 :]
        pairs = [pair_add(pairs[i], pairs[i + 1]) for i in range(0, len(pairs) - 1, 2)] + tail
    return pairs[0]


def pair_total(pairs):
    total = pair_tree(pairs)
    for by in (4, 2, 1):
        total = pair_add(total, tuple(pltpu.roll(v, by, 0) for v in total))
    return total


def sweep_kernel(x_ref, f_ref, c_ref, halo_ref, a_ref, b_ref, out_x_ref, out_r_ref, pair_ref, d_s, r_s, c_s):
    odd_x = is_odd("bx")
    rows, cols = x_ref.shape
    n = FIELDS * SUB
    tiles, inner = d_s.shape[0] // SUB, rows // SUB
    wide = cols + LANE
    high = d_s.shape[0]
    a, b = a_ref[...], b_ref[...]
    left, right = jnp.where(odd_x, a, b), jnp.where(odd_x, b, a)
    pieces = []
    for f in range(FIELDS):
        at = slice(f * SUB, (f + 1) * SUB)
        pieces += [left[at], right[at]]
    pieces.append(jnp.zeros((LANE - 2 * n, a.shape[1]), jnp.float32))
    sides = jnp.concatenate(pieces, axis=0).T
    for f, (ref, main) in enumerate(((d_s, x_ref), (r_s, f_ref), (c_s, c_ref))):
        at = slice(f * SUB, (f + 1) * SUB)
        ref[0:rows, 0:cols] = main[...]
        ref[rows : rows + SUB, 0:cols] = halo_ref[at, :]
        ref[rows + SUB : high, 0:cols] = halo_ref[n + f * SUB : n + (f + 1) * SUB, :]
        ref[:, cols:wide] = pltpu.roll(sides[0:high], LANE - (2 * f + 1) * SUB, 1)

    theta, steps = coefficients()
    row_id = lax.broadcasted_iota(jnp.int32, (SUB, wide), 0)
    first_row, last_row = row_id == 0, row_id == SUB - 1

    def across(i):
        v = d_s[i * SUB : (i + 1) * SUB, :]
        pair = pltpu.roll(v, 1, 1) + pltpu.roll(v, wide - 1, 1)
        mixed = v + 0.5 * pair
        return v, pair, pltpu.roll(mixed, 1, 0), pltpu.roll(mixed, SUB - 1, 0)

    squares = []
    for sweep in range(ITERS + 1):
        head, tail = across(0), across(tiles - 1)
        before, now = tail, head
        for i in range(tiles):
            if i < tiles - 2:
                after = across(i + 1)
            else:
                after = tail if i == tiles - 2 else head
            v, pair, down, up = now
            from_below = jnp.where(first_row, before[2], down)
            from_above = jnp.where(last_row, after[3], up)
            at = slice(i * SUB, (i + 1) * SUB)
            c = c_s[at, :]
            image = jnp.where(c > 0.0, c * v - (pair + (from_below + from_above)), jnp.zeros_like(c))
            r = r_s[at, :] - image
            if sweep < ITERS:
                r_s[at, :] = r
                if sweep == 0:
                    d = r * (1.0 / theta)
                else:
                    keep, gain = steps[sweep - 1]
                    d = keep * v + gain * r
                d_s[at, :] = d
                if i < inner:
                    old = x_ref[at, :] if sweep == 0 else out_x_ref[at, :]
                    out_x_ref[at, :] = old + d[:, :cols]
            elif i < inner:
                r = r[:, :cols]
                out_r_ref[at, :] = r
                squares.append(jnp.sum(r * r, axis=1, keepdims=True))
            before, now = now, after
    zero = jnp.zeros_like(squares[0])
    upper, lower = pair_total([(q, zero) for q in squares])
    lane = lax.broadcasted_iota(jnp.int32, (SUB, LANE), 1)
    tile = jnp.where(lane < LANE // 2, upper, lower)
    for i in range(pair_ref.shape[0] // SUB):
        pair_ref[i * SUB : (i + 1) * SUB, :] = tile


def norm_kernel(cells, pairs_ref, out_ref):
    pairs = []
    for i in range(pairs_ref.shape[0] // SUB):
        upper = pairs_ref[i * SUB : (i + 1) * SUB, :]
        pairs.append((upper, pltpu.roll(upper, LANE // 2, 1)))
    upper, lower = pair_total(pairs)
    out_ref[0] = jnp.sqrt((upper + lower) * (1.0 / cells))[0, 0]


def swap(value, mesh_shape, partner):
    wide, high = mesh_shape
    moves = []
    for b in range(wide):
        for j in range(high):
            other = partner(b, j)
            if other is not None:
                moves.append((b * high + j, other[0] * high + other[1]))
    return lax.ppermute(value, ("bx", "by"), moves)


def per_device(forcing, guess, shift, ocean):
    rows, cols = forcing.shape
    wide, high = lax.axis_size("bx"), lax.axis_size("by")
    devices = wide * high
    assert rows % SUB == 0 and cols % LANE == 0 and devices % SUB == 0
    assert wide % 2 == 0 and high % 2 == 0
    n = FIELDS * SUB
    tall = rows + 2 * SUB
    span = -(-tall // LANE) * LANE
    f32 = functools.partial(jax.ShapeDtypeStruct, dtype=jnp.float32)
    held = functools.partial(pltpu.VMEM, dtype=jnp.float32)
    fields = [pltpu.with_memory_space_constraint(v, pltpu.HBM) for v in (forcing, guess, shift, ocean)]
    edges = [pltpu.VMEM((SUB, cols), v.dtype) for v in fields]
    near, far = call(
        edge_kernel,
        (f32((n, cols)),) * 2,
        [HBM] * 4,
        (VMEM,) * 2,
        edges * 2 + [pltpu.SemaphoreType.DMA((8,))],
    )(*fields)

    def own_chip(b, j):
        return (b, j ^ 1)

    def next_chip(b, j):
        if j == 0:
            return None
        if j == high - 1:
            return (wide - 1 - b, j)
        return (b, ((j - 1) ^ 1) + 1)

    def even_pair(b, j):
        return (b ^ 1, j)

    def odd_pair(b, j):
        return ((((b - 1) % wide) ^ 1) + 1) % wide, j

    shape = (wide, high)
    near = swap(near, shape, own_chip)
    far = swap(far, shape, next_chip)
    x, f, c, columns = call(
        block_kernel,
        (f32((rows, cols)),) * 3 + (f32((2 * n, span)),),
        [HBM] * 4,
        (VMEM,) * 4,
        [pltpu.VMEM((rows, cols), v.dtype) for v in fields] + [pltpu.SemaphoreType.DMA((4,))],
    )(*fields)
    halo, a, b = call(
        functools.partial(halo_kernel, rows),
        (f32((2 * n, cols)), f32((n, span)), f32((n, span))),
        [VMEM] * 3,
        (VMEM,) * 3,
    )(near, far, columns)
    a = swap(a, shape, even_pair)
    b = swap(b, shape, odd_pair)
    x, r, pairs = call(
        sweep_kernel,
        (held((rows, cols)), held((rows, cols)), held((devices, LANE))),
        [VMEM] * 6,
        (VMEM,) * 3,
        [pltpu.VMEM((tall, cols + LANE), jnp.float32)] * 3,
    )(x, f, c, halo, a, b)
    pairs = lax.all_to_all(pairs, ("bx", "by"), 0, 0, tiled=True)
    cells = rows * cols * devices
    norm = call(functools.partial(norm_kernel, cells), f32((1,)), [VMEM], SMEM)(pairs)
    return (x, r, norm[0])


def solution(mesh):
    spec = P("by", "bx")
    return jax.shard_map(
        per_device, mesh=mesh, in_specs=(spec,) * 4, out_specs=(spec, spec, P()), check_vma=False
    )
```

```python
import functools

import jax
import jax.numpy as jnp
from jax import lax
from jax.experimental import pallas as pl
from jax.experimental.pallas import tpu as pltpu
from jax.sharding import PartitionSpec as P

ITERS = 4
LOW_BOUND = 0.05
HIGH_BOUND = 14.5

SUB = 8
LANE = 128
FIELDS = 3
VMEM = pl.BlockSpec(memory_space=pltpu.VMEM)
SMEM = pl.BlockSpec(memory_space=pltpu.SMEM)
HBM = pl.BlockSpec(memory_space=pltpu.HBM)
GRANT = pltpu.CompilerParams(vmem_limit_bytes=8 << 20)


def call(kernel, shapes, in_specs, out_specs, scratch=(), flops=100000):
    return pl.pallas_call(
        kernel,
        out_shape=shapes,
        in_specs=in_specs,
        out_specs=out_specs,
        scratch_shapes=scratch,
        cost_estimate=pl.CostEstimate(flops=flops, bytes_accessed=0, transcendentals=0),
        compiler_params=GRANT,
    )


def masked_fields(forcing, guess, shift, ocean):
    zero = jnp.zeros_like(forcing)
    sea = ocean > 0
    return (
        jnp.where(sea, guess, zero),
        jnp.where(sea, forcing, zero),
        jnp.where(sea, 6.0 + shift, zero),
    )


def is_odd(axis):
    return lax.rem(lax.axis_index(axis), 2) == 1


def edge_kernel(*refs):
    near_ref, far_ref = refs[4:6]
    low_s, top_s = refs[6:10], refs[10:14]
    sem = refs[14]
    rows = refs[0].shape[0]
    copies = []
    for i in range(4):
        copies.append(pltpu.make_async_copy(refs[i].at[0:SUB, :], low_s[i], sem.at[2 * i]))
        copies.append(pltpu.make_async_copy(refs[i].at[rows - SUB : rows, :], top_s[i], sem.at[2 * i + 1]))
    for copy in copies:
        copy.start()
    odd = is_odd("by")
    for copy in copies:
        copy.wait()
    low = masked_fields(*(ref[...] for ref in low_s))
    top = masked_fields(*(ref[...] for ref in top_s))
    for f in range(FIELDS):
        at = slice(f * SUB, (f + 1) * SUB)
        near_ref[at, :] = jnp.where(odd, low[f], top[f])
        far_ref[at, :] = jnp.where(odd, top[f], low[f])


def pack_columns(fields):
    rows, cols = fields[0].shape
    lane = lax.broadcasted_iota(jnp.int32, (rows, LANE), 1)
    packed = jnp.zeros((rows, LANE), jnp.float32)
    for f, field in enumerate(fields):
        at = f * SUB
        left = field[:, :LANE]
        left = pltpu.roll(left, at, 1) if at else left
        packed = jnp.where((lane >= at) & (lane < at + SUB), left, packed)
        at = (FIELDS + f) * SUB
        right = pltpu.roll(field[:, cols - LANE :], at + SUB, 1)
        packed = jnp.where((lane >= at) & (lane < at + SUB), right, packed)
    return packed


def block_kernel(*refs):
    x_ref, r_ref, c_ref, columns_ref = refs[4:8]
    held, sem = refs[8:12], refs[12]
    copies = [pltpu.make_async_copy(refs[i], held[i], sem.at[i]) for i in range(4)]
    for copy in copies:
        copy.start()
    for copy in copies:
        copy.wait()
    fields = masked_fields(*(ref[...] for ref in held))
    for ref, field in zip((x_ref, r_ref, c_ref), fields):
        ref[...] = field
    packed = pack_columns(fields)
    width = columns_ref.shape[1]
    packed = jnp.concatenate([packed, jnp.zeros((width - packed.shape[0], LANE), jnp.float32)], axis=0)
    columns_ref[...] = packed.T[: 2 * FIELDS * SUB]


def mirrored(tile):
    back = LANE - 1 - lax.broadcasted_iota(jnp.int32, (SUB, LANE), 1)
    up = SUB - 1 - lax.broadcasted_iota(jnp.int32, (SUB, LANE), 0)
    parts = []
    for at in reversed(range(0, tile.shape[1], LANE)):
        part = jnp.take_along_axis(tile[:, at : at + LANE], back, axis=1)
        parts.append(jnp.take_along_axis(part, up, axis=0))
    return jnp.concatenate(parts, axis=1)


def halo_kernel(rows, near_ref, far_ref, columns_ref, halo_ref, a_ref, b_ref):
    odd, odd_x = is_odd("by"), is_odd("bx")
    fold = lax.axis_index("by") == lax.axis_size("by") - 1
    n = FIELDS * SUB
    near, far = near_ref[...], far_ref[...]
    halo_ref[0:n, :] = jnp.where(odd, far, near)
    halo_ref[n : 2 * n, :] = jnp.where(odd, near, far)

    @pl.when(fold)
    def _():
        for f in range(FIELDS):
            at = slice(f * SUB, (f + 1) * SUB)
            halo_ref[at, :] = mirrored(halo_ref[at, :])

    fields = [
        jnp.concatenate([halo_ref[f * SUB : (f + 1) * SUB, :], halo_ref[n + f * SUB : n + (f + 1) * SUB, :]], axis=0)
        for f in range(FIELDS)
    ]
    packed = pack_columns(fields)
    width = columns_ref.shape[1]
    start = rows // LANE * LANE
    before, after = rows - start, width - rows - 2 * SUB
    pieces = [packed]
    if before:
        pieces.insert(0, jnp.zeros((before, LANE), jnp.float32))
    if after:
        pieces.append(jnp.zeros((after, LANE), jnp.float32))
    ends = jnp.concatenate(pieces, axis=0).T[: 2 * n]
    for at, first, second in ((slice(0, start), None, None), (slice(start, width), ends[:n], ends[n:])):
        if at.stop == at.start:
            continue
        left, right = columns_ref[0:n, at], columns_ref[n : 2 * n, at]
        if first is not None:
            left, right = left + first, right + second
        a_ref[:, at] = jnp.where(odd_x, left, right)
        b_ref[:, at] = jnp.where(odd_x, right, left)


def coefficients():
    theta = (HIGH_BOUND + LOW_BOUND) / 2.0
    delta = (HIGH_BOUND - LOW_BOUND) / 2.0
    sigma = theta / delta
    rho = 1.0 / sigma
    steps = []
    for _ in range(ITERS):
        following = 1.0 / (2.0 * sigma - rho)
        steps.append((following * rho, 2.0 * following / delta))
        rho = following
    return theta, steps


def pair_add(first, second):
    total = first[0] + second[0]
    backed = total - first[0]
    error = first[0] - (total - backed) + (second[0] - backed)
    error = error + first[1] + second[1]
    upper = total + error
    lower = error - (upper - total)
    return (upper, lower)


def pair_tree(pairs):
    while len(pairs) > 1:
        tail = pairs[len(pairs) // 2 * 2 :]
        pairs = [pair_add(pairs[i], pairs[i + 1]) for i in range(0, len(pairs) - 1, 2)] + tail
    return pairs[0]


def pair_total(pairs):
    total = pair_tree(pairs)
    for by in (4, 2, 1):
        total = pair_add(total, tuple(pltpu.roll(v, by, 0) for v in total))
    return total


def sweeps(inner, x_s, d_s, r_s, c_s, weigh):
    tall, wide = d_s.shape
    tiles = tall // SUB
    theta, steps = coefficients()
    row_id = lax.broadcasted_iota(jnp.int32, (SUB, wide), 0)
    first_row, last_row = row_id == 0, row_id == SUB - 1

    def across(i):
        v = d_s[i * SUB : (i + 1) * SUB, :]
        pair = pltpu.roll(v, 1, 1) + pltpu.roll(v, wide - 1, 1)
        mixed = v + 0.5 * pair
        return v, pair, pltpu.roll(mixed, 1, 0), pltpu.roll(mixed, SUB - 1, 0)

    squares = []
    for sweep in range(ITERS + 1):
        head, tail = across(0), across(tiles - 1)
        before, now = tail, head
        for i in range(tiles):
            if i < tiles - 2:
                after = across(i + 1)
            else:
                after = tail if i == tiles - 2 else head
            v, pair, down, up = now
            from_below = jnp.where(first_row, before[2], down)
            from_above = jnp.where(last_row, after[3], up)
            at = slice(i * SUB, (i + 1) * SUB)
            c = c_s[at, :]
            image = jnp.where(c > 0.0, c * v - (pair + (from_below + from_above)), jnp.zeros_like(c))
            r = r_s[at, :] - image
            if sweep < ITERS:
                r_s[at, :] = r
                if sweep == 0:
                    d = r * (1.0 / theta)
                else:
                    keep, gain = steps[sweep - 1]
                    d = keep * v + gain * r
                d_s[at, :] = d
                if i < inner:
                    x_s[at, :] = (v if sweep == 0 else x_s[at, :]) + d
            elif i < inner:
                r_s[at, :] = r
                r = jnp.where(weigh, r, jnp.zeros_like(r))
                squares.append(jnp.sum(r * r, axis=1, keepdims=True))
            before, now = now, after
    zero = jnp.zeros_like(squares[0])
    return pair_total([(q, zero) for q in squares])


def interior_kernel(x_ref, f_ref, c_ref, halo_ref, out_x_ref, out_r_ref, pair_ref, strip_x, strip_r, strip_c, d_s, c_s):
    rows, cols = x_ref.shape
    high = d_s.shape[0]
    n = FIELDS * SUB
    lane = lax.broadcasted_iota(jnp.int32, (high, LANE), 1)
    left, right = (lane >= LANE // 2) & (lane < LANE // 2 + 2 * SUB), lane >= LANE - 2 * SUB
    for f, (ref, main, strip) in enumerate(((d_s, x_ref, strip_x), (out_r_ref, f_ref, strip_r), (c_s, c_ref, strip_c))):
        ref[0:rows, :] = main[...]
        ref[rows : rows + SUB, :] = halo_ref[f * SUB : (f + 1) * SUB, :]
        ref[rows + SUB : high, :] = halo_ref[n + f * SUB : n + (f + 1) * SUB, :]
        ends = jnp.where(left, pltpu.roll(ref[:, 0:LANE], LANE // 2, 1), 0.0)
        strip[...] = jnp.where(right, ref[:, cols - LANE : cols], ends)
    column = lax.broadcasted_iota(jnp.int32, (SUB, cols), 1)
    weigh = (column >= SUB) & (column < cols - SUB)
    upper, lower = sweeps(rows // SUB, out_x_ref, d_s, out_r_ref, c_s, weigh)
    pair_ref[0:SUB, :] = jnp.broadcast_to(upper, (SUB, LANE))
    pair_ref[SUB : 2 * SUB, :] = jnp.broadcast_to(lower, (SUB, LANE))


def strip_kernel(strip_x, strip_r, strip_c, a_ref, b_ref, pair_ref, out_x_ref, out_r_ref, pairs_ref, d_s, c_s):
    odd_x = is_odd("bx")
    high = d_s.shape[0]
    n = FIELDS * SUB
    middle = LANE // 2
    a, b = a_ref[...], b_ref[...]
    left, right = jnp.where(odd_x, a, b), jnp.where(odd_x, b, a)
    gap = jnp.zeros((middle - SUB - n, a.shape[1]), jnp.float32)
    rest = jnp.zeros((middle + SUB - n, a.shape[1]), jnp.float32)
    sides = jnp.concatenate([right, gap, left, rest], axis=0).T[0:high]
    lane = lax.broadcasted_iota(jnp.int32, (high, LANE), 1)
    ghost = (lane < SUB) | ((lane >= middle - SUB) & (lane < middle))
    for f, (ref, strip) in enumerate(((d_s, strip_x), (out_r_ref, strip_r), (c_s, strip_c))):
        side = pltpu.roll(sides, LANE - f * SUB, 1) if f else sides
        ref[...] = jnp.where(ghost, side, strip[...])
    lane = lax.broadcasted_iota(jnp.int32, (SUB, LANE), 1)
    weigh = ((lane >= middle) & (lane < middle + SUB)) | (lane >= LANE - SUB)
    ends = sweeps(out_x_ref.shape[0] // SUB, out_x_ref, d_s, out_r_ref, c_s, weigh)
    upper, lower = pair_add(ends, (pair_ref[0:SUB, :], pair_ref[SUB : 2 * SUB, :]))
    tile = jnp.where(lane < middle, upper, lower)
    for i in range(pairs_ref.shape[0] // SUB):
        pairs_ref[i * SUB : (i + 1) * SUB, :] = tile


def norm_kernel(cells, pairs_ref, x_ref, r_ref, strip_x, strip_r, x_hbm, r_hbm, norm_ref, x_s, r_s, sem):
    rows, cols = x_s.shape
    lane = lax.broadcasted_iota(jnp.int32, (rows, LANE), 1)
    copies = []
    for i, (main, strip, joined, out) in enumerate(((x_ref, strip_x, x_s, x_hbm), (r_ref, strip_r, r_s, r_hbm))):
        joined[...] = main[0:rows, :]
        ends = strip[0:rows, :]
        joined[:, 0:LANE] = jnp.where(lane < SUB, pltpu.roll(ends, LANE // 2, 1), joined[:, 0:LANE])
        joined[:, cols - LANE : cols] = jnp.where(lane >= LANE - SUB, ends, joined[:, cols - LANE : cols])
        copies.append(pltpu.make_async_copy(joined, out, sem.at[i]))
        copies[i].start()
    pairs = []
    for i in range(pairs_ref.shape[0] // SUB):
        upper = pairs_ref[i * SUB : (i + 1) * SUB, :]
        pairs.append((upper, pltpu.roll(upper, LANE // 2, 1)))
    upper, lower = pair_total(pairs)
    norm_ref[0] = jnp.sqrt((upper + lower) * (1.0 / cells))[0, 0]
    for copy in copies:
        copy.wait()


def swap(value, mesh_shape, partner):
    wide, high = mesh_shape
    moves = []
    for b in range(wide):
        for j in range(high):
            other = partner(b, j)
            if other is not None:
                moves.append((b * high + j, other[0] * high + other[1]))
    return lax.ppermute(value, ("bx", "by"), moves)


def per_device(forcing, guess, shift, ocean):
    rows, cols = forcing.shape
    wide, high = lax.axis_size("bx"), lax.axis_size("by")
    devices = wide * high
    assert rows % SUB == 0 and cols % LANE == 0 and devices % SUB == 0
    assert wide % 2 == 0 and high % 2 == 0
    n = FIELDS * SUB
    tall = rows + 2 * SUB
    span = -(-tall // LANE) * LANE
    f32 = functools.partial(jax.ShapeDtypeStruct, dtype=jnp.float32)
    held = functools.partial(pltpu.VMEM, dtype=jnp.float32)
    fields = [pltpu.with_memory_space_constraint(v, pltpu.HBM) for v in (forcing, guess, shift, ocean)]
    edges = [pltpu.VMEM((SUB, cols), v.dtype) for v in fields]
    near, far = call(
        edge_kernel,
        (f32((n, cols)),) * 2,
        [HBM] * 4,
        (VMEM,) * 2,
        edges * 2 + [pltpu.SemaphoreType.DMA((8,))],
    )(*fields)

    def own_chip(b, j):
        return (b, j ^ 1)

    def next_chip(b, j):
        if j == 0:
            return None
        if j == high - 1:
            return (wide - 1 - b, j)
        return (b, ((j - 1) ^ 1) + 1)

    def even_pair(b, j):
        return (b ^ 1, j)

    def odd_pair(b, j):
        return ((((b - 1) % wide) ^ 1) + 1) % wide, j

    shape = (wide, high)
    near = swap(near, shape, own_chip)
    far = swap(far, shape, next_chip)
    x, f, c, columns = call(
        block_kernel,
        (f32((rows, cols)),) * 3 + (f32((2 * n, span)),),
        [HBM] * 4,
        (VMEM,) * 4,
        [pltpu.VMEM((rows, cols), v.dtype) for v in fields] + [pltpu.SemaphoreType.DMA((4,))],
    )(*fields)
    halo, a, b = call(
        functools.partial(halo_kernel, rows),
        (f32((2 * n, cols)), f32((n, span)), f32((n, span))),
        [VMEM] * 3,
        (VMEM,) * 3,
    )(near, far, columns)
    a = swap(a, shape, even_pair)
    b = swap(b, shape, odd_pair)
    high = (tall, LANE)
    x, r, pair, *strips = call(
        interior_kernel,
        (held((rows, cols)), held((tall, cols)), held((2 * SUB, LANE))) + (held(high),) * 3,
        [VMEM] * 4,
        (VMEM,) * 6,
        [pltpu.VMEM((tall, cols), jnp.float32)] * 2,
    )(x, f, c, halo)
    strip_x, strip_r, pairs = call(
        strip_kernel,
        (held((rows, LANE)), held(high), held((devices, LANE))),
        [VMEM] * 6,
        (VMEM,) * 3,
        [pltpu.VMEM(high, jnp.float32)] * 2,
    )(*strips, a, b, pair)
    pairs = lax.all_to_all(pairs, ("bx", "by"), 0, 0, tiled=True)
    x, r, norm = call(
        functools.partial(norm_kernel, rows * cols * devices),
        (f32((rows, cols)), f32((rows, cols)), f32((1,))),
        [VMEM] * 5,
        (HBM, HBM, SMEM),
        [pltpu.VMEM((rows, cols), jnp.float32)] * 2 + [pltpu.SemaphoreType.DMA((2,))],
    )(pairs, x, r, strip_x, strip_r)
    return (x, r, norm[0])


def solution(mesh):
    spec = P("by", "bx")
    return jax.shard_map(
        per_device, mesh=mesh, in_specs=(spec,) * 4, out_specs=(spec, spec, P()), check_vma=False
    )
```

```python
import functools

import jax
import jax.numpy as jnp
from jax import lax
from jax.experimental import pallas as pl
from jax.experimental.pallas import tpu as pltpu
from jax.sharding import PartitionSpec as P

ITERS = 4
LOW_BOUND = 0.05
HIGH_BOUND = 14.5

SUB = 8
LANE = 128
FIELDS = 3
DEPTH = ITERS + 1
COLUMNS = 2 * SUB
LEFT = LANE // 2 - SUB + DEPTH
VMEM = pl.BlockSpec(memory_space=pltpu.VMEM)
HBM = pl.BlockSpec(memory_space=pltpu.HBM)
GRANT = pltpu.CompilerParams(vmem_limit_bytes=8 << 20)


def call(kernel, shapes, in_specs, out_specs, scratch=(), flops=100000):
    return pl.pallas_call(
        kernel,
        out_shape=shapes,
        in_specs=in_specs,
        out_specs=out_specs,
        scratch_shapes=scratch,
        cost_estimate=pl.CostEstimate(flops=flops, bytes_accessed=0, transcendentals=0),
        compiler_params=GRANT,
    )


def masked_fields(forcing, guess, shift, ocean):
    zero = jnp.zeros_like(forcing)
    sea = ocean > 0
    return (
        jnp.where(sea, guess, zero),
        jnp.where(sea, forcing, zero),
        jnp.where(sea, 6.0 + shift, zero),
    )


def is_odd(axis):
    return lax.rem(lax.axis_index(axis), 2) == 1


def edge_kernel(*refs):
    near_ref, far_ref = refs[4:6]
    low_s, top_s = refs[6:10], refs[10:14]
    sem = refs[14]
    rows = refs[0].shape[0]
    copies = []
    for i in range(4):
        copies.append(pltpu.make_async_copy(refs[i].at[0:SUB, :], low_s[i], sem.at[2 * i]))
        copies.append(pltpu.make_async_copy(refs[i].at[rows - SUB : rows, :], top_s[i], sem.at[2 * i + 1]))
    for copy in copies:
        copy.start()
    odd = is_odd("by")
    for copy in copies:
        copy.wait()
    low = masked_fields(*(ref[...] for ref in low_s))
    top = masked_fields(*(ref[...] for ref in top_s))
    for f in range(FIELDS):
        at = slice(f * SUB, (f + 1) * SUB)
        near_ref[at, :] = jnp.where(odd, low[f], top[f])
        far_ref[at, :] = jnp.where(odd, top[f], low[f])


def pack_columns(fields):
    rows, cols = fields[0].shape
    lane = lax.broadcasted_iota(jnp.int32, (rows, LANE), 1)
    packed = jnp.zeros((rows, LANE), jnp.float32)
    for f, field in enumerate(fields):
        at = f * DEPTH
        left = field[:, :LANE]
        left = pltpu.roll(left, at, 1) if at else left
        packed = jnp.where((lane >= at) & (lane < at + DEPTH), left, packed)
        at = COLUMNS + f * DEPTH
        right = pltpu.roll(field[:, cols - LANE :], at + DEPTH, 1)
        packed = jnp.where((lane >= at) & (lane < at + DEPTH), right, packed)
    return packed


def block_kernel(*refs):
    x_ref, r_ref, c_ref, columns_ref = refs[4:8]
    held, sem = refs[8:12], refs[12]
    copies = [pltpu.make_async_copy(refs[i], held[i], sem.at[i]) for i in range(4)]
    for copy in copies:
        copy.start()
    for copy in copies:
        copy.wait()
    fields = masked_fields(*(ref[...] for ref in held))
    for ref, field in zip((x_ref, r_ref, c_ref), fields):
        ref[...] = field
    packed = pack_columns(fields)
    width = columns_ref.shape[1]
    packed = jnp.concatenate([packed, jnp.zeros((width - packed.shape[0], LANE), jnp.float32)], axis=0)
    columns_ref[...] = packed.T[: 2 * COLUMNS]


def mirrored(tile):
    back = LANE - 1 - lax.broadcasted_iota(jnp.int32, (SUB, LANE), 1)
    up = SUB - 1 - lax.broadcasted_iota(jnp.int32, (SUB, LANE), 0)
    parts = []
    for at in reversed(range(0, tile.shape[1], LANE)):
        part = jnp.take_along_axis(tile[:, at : at + LANE], back, axis=1)
        parts.append(jnp.take_along_axis(part, up, axis=0))
    return jnp.concatenate(parts, axis=1)


def halo_kernel(rows, far_ref, near_ref, columns_ref, halo_ref, a_ref, b_ref):
    odd, odd_x = is_odd("by"), is_odd("bx")
    fold = lax.axis_index("by") == lax.axis_size("by") - 1
    n = FIELDS * SUB
    near, far = near_ref[...], far_ref[...]
    halo_ref[0:n, :] = jnp.where(odd, far, near)
    halo_ref[n : 2 * n, :] = jnp.where(odd, near, far)

    @pl.when(fold)
    def _():
        for f in range(FIELDS):
            at = slice(f * SUB, (f + 1) * SUB)
            halo_ref[at, :] = mirrored(halo_ref[at, :])

    fields = [
        jnp.concatenate([halo_ref[f * SUB : (f + 1) * SUB, :], halo_ref[n + f * SUB : n + (f + 1) * SUB, :]], axis=0)
        for f in range(FIELDS)
    ]
    packed = pack_columns(fields)
    width = columns_ref.shape[1]
    start = width - LANE
    before, after = rows - start, width - rows - 2 * SUB
    pieces = [packed]
    if before:
        pieces.insert(0, jnp.zeros((before, LANE), jnp.float32))
    if after:
        pieces.append(jnp.zeros((after, LANE), jnp.float32))
    rest = columns_ref[:, start:width] + jnp.concatenate(pieces, axis=0).T[: 2 * COLUMNS]
    sides = []
    for at in (slice(0, COLUMNS), slice(COLUMNS, 2 * COLUMNS)):
        parts = [columns_ref[at, p : p + LANE] for p in range(0, start, LANE)]
        sides.append(jnp.concatenate(parts + [folded(rest[at])], axis=0))
    a_ref[...] = jnp.where(odd_x, sides[0], sides[1])
    b_ref[...] = jnp.where(odd_x, sides[1], sides[0])


def folded(rest):
    return rest[0:SUB] + pltpu.roll(rest[SUB:COLUMNS], LANE // 2, 1)


def unfolded(value):
    parts = [value[p : p + COLUMNS] for p in range(0, value.shape[0] - SUB, COLUMNS)]
    rest = value[value.shape[0] - SUB :]
    parts.append(jnp.concatenate([rest, pltpu.roll(rest, LANE // 2, 1)], axis=0))
    return jnp.concatenate(parts, axis=1)


def coefficients():
    theta = (HIGH_BOUND + LOW_BOUND) / 2.0
    delta = (HIGH_BOUND - LOW_BOUND) / 2.0
    sigma = theta / delta
    rho = 1.0 / sigma
    steps = []
    for _ in range(ITERS):
        following = 1.0 / (2.0 * sigma - rho)
        steps.append((following * rho, 2.0 * following / delta))
        rho = following
    return theta, steps


def pair_add(first, second):
    total = first[0] + second[0]
    backed = total - first[0]
    error = first[0] - (total - backed) + (second[0] - backed)
    error = error + first[1] + second[1]
    upper = total + error
    lower = error - (upper - total)
    return (upper, lower)


def pair_tree(pairs):
    while len(pairs) > 1:
        tail = pairs[len(pairs) // 2 * 2 :]
        pairs = [pair_add(pairs[i], pairs[i + 1]) for i in range(0, len(pairs) - 1, 2)] + tail
    return pairs[0]


def pair_total(pairs):
    total = pair_tree(pairs)
    for by in (4, 2, 1):
        total = pair_add(total, tuple(pltpu.roll(v, by, 0) for v in total))
    return total


def sweeps(inner, x_s, d_s, r_s, c_s, weigh):
    tall, wide = d_s.shape
    tiles = tall // SUB
    theta, steps = coefficients()
    row_id = lax.broadcasted_iota(jnp.int32, (SUB, wide), 0)
    first_row, last_row = row_id == 0, row_id == SUB - 1

    def across(i):
        v = d_s[i * SUB : (i + 1) * SUB, :]
        pair = pltpu.roll(v, 1, 1) + pltpu.roll(v, wide - 1, 1)
        mixed = v + 0.5 * pair
        return v, pair, pltpu.roll(mixed, 1, 0), pltpu.roll(mixed, SUB - 1, 0)

    squares = []
    for sweep in range(ITERS + 1):
        head, tail = across(0), across(tiles - 1)
        before, now = tail, head
        for i in range(tiles):
            if i < tiles - 2:
                after = across(i + 1)
            else:
                after = tail if i == tiles - 2 else head
            v, pair, down, up = now
            from_below = jnp.where(first_row, before[2], down)
            from_above = jnp.where(last_row, after[3], up)
            at = slice(i * SUB, (i + 1) * SUB)
            c = c_s[at, :]
            image = jnp.where(c > 0.0, c * v - (pair + (from_below + from_above)), jnp.zeros_like(c))
            r = r_s[at, :] - image
            if sweep < ITERS:
                r_s[at, :] = r
                if sweep == 0:
                    d = r * (1.0 / theta)
                else:
                    keep, gain = steps[sweep - 1]
                    d = keep * v + gain * r
                d_s[at, :] = d
                if i < inner:
                    x_s[at, :] = (v if sweep == 0 else x_s[at, :]) + d
            elif i < inner:
                r_s[at, :] = r
                r = jnp.where(weigh, r, jnp.zeros_like(r))
                squares.append(jnp.sum(r * r, axis=1, keepdims=True))
            before, now = now, after
    zero = jnp.zeros_like(squares[0])
    return pair_total([(q, zero) for q in squares])


def interior_kernel(x_ref, f_ref, c_ref, halo_ref, out_x_ref, out_r_ref, pair_ref, strip_x, strip_r, strip_c, d_s, c_s):
    rows, cols = x_ref.shape
    high = d_s.shape[0]
    n = FIELDS * SUB
    lane = lax.broadcasted_iota(jnp.int32, (high, LANE), 1)
    left, right = (lane >= LEFT) & (lane < LEFT + 2 * SUB), lane >= LANE - 2 * SUB
    for f, (ref, main, strip) in enumerate(((d_s, x_ref, strip_x), (out_r_ref, f_ref, strip_r), (c_s, c_ref, strip_c))):
        ref[0:rows, :] = main[...]
        ref[rows : rows + SUB, :] = halo_ref[f * SUB : (f + 1) * SUB, :]
        ref[rows + SUB : high, :] = halo_ref[n + f * SUB : n + (f + 1) * SUB, :]
        ends = jnp.where(left, pltpu.roll(ref[:, 0:LANE], LEFT, 1), 0.0)
        strip[...] = jnp.where(right, ref[:, cols - LANE : cols], ends)
    column = lax.broadcasted_iota(jnp.int32, (SUB, cols), 1)
    weigh = (column >= SUB) & (column < cols - SUB)
    upper, lower = sweeps(rows // SUB, out_x_ref, d_s, out_r_ref, c_s, weigh)
    pair_ref[0:SUB, :] = jnp.broadcast_to(upper, (SUB, LANE))
    pair_ref[SUB : 2 * SUB, :] = jnp.broadcast_to(lower, (SUB, LANE))


def strip_kernel(strip_x, strip_r, strip_c, b_ref, a_ref, pair_ref, out_x_ref, out_r_ref, pairs_ref, d_s, c_s):
    odd_x = is_odd("bx")
    high = d_s.shape[0]
    a, b = unfolded(a_ref[...]), unfolded(b_ref[...])
    left, right = jnp.where(odd_x, a, b), jnp.where(odd_x, b, a)
    start = LEFT - DEPTH
    gap = jnp.zeros((start - COLUMNS, a.shape[1]), jnp.float32)
    rest = jnp.zeros((LANE - start - COLUMNS, a.shape[1]), jnp.float32)
    sides = jnp.concatenate([right, gap, left, rest], axis=0).T[0:high]
    lane = lax.broadcasted_iota(jnp.int32, (high, LANE), 1)
    ghost = (lane < DEPTH) | ((lane >= start) & (lane < LEFT))
    for f, (ref, strip) in enumerate(((d_s, strip_x), (out_r_ref, strip_r), (c_s, strip_c))):
        side = pltpu.roll(sides, LANE - f * DEPTH, 1) if f else sides
        ref[...] = jnp.where(ghost, side, strip[...])
    lane = lax.broadcasted_iota(jnp.int32, (SUB, LANE), 1)
    weigh = ((lane >= LEFT) & (lane < LEFT + SUB)) | (lane >= LANE - SUB)
    ends = sweeps(out_x_ref.shape[0] // SUB, out_x_ref, d_s, out_r_ref, c_s, weigh)
    upper, lower = pair_add(ends, (pair_ref[0:SUB, :], pair_ref[SUB : 2 * SUB, :]))
    tile = jnp.where(lane < LANE // 2, upper, lower)
    for i in range(pairs_ref.shape[0] // SUB):
        pairs_ref[i * SUB : (i + 1) * SUB, :] = tile


def norm_kernel(cells, pairs_ref, x_ref, r_ref, strip_x, strip_r, x_hbm, r_hbm, norm_hbm, x_s, r_s, norm_s, sem):
    rows, cols = x_s.shape
    lane = lax.broadcasted_iota(jnp.int32, (rows, LANE), 1)
    copies = []
    for i, (main, strip, joined, out) in enumerate(((x_ref, strip_x, x_s, x_hbm), (r_ref, strip_r, r_s, r_hbm))):
        joined[...] = main[0:rows, :]
        ends = strip[0:rows, :]
        joined[:, 0:LANE] = jnp.where(lane < SUB, pltpu.roll(ends, LANE - LEFT, 1), joined[:, 0:LANE])
        joined[:, cols - LANE : cols] = jnp.where(lane >= LANE - SUB, ends, joined[:, cols - LANE : cols])
        copies.append(pltpu.make_async_copy(joined, out, sem.at[i]))
        copies[i].start()
    pairs = []
    for i in range(pairs_ref.shape[0] // SUB):
        upper = pairs_ref[i * SUB : (i + 1) * SUB, :]
        pairs.append((upper, pltpu.roll(upper, LANE // 2, 1)))
    upper, lower = pair_total(pairs)
    norm_s[0] = jnp.sqrt((upper + lower) * (1.0 / cells))[0, 0]
    copies.append(pltpu.make_async_copy(norm_s, norm_hbm, sem.at[2]))
    copies[2].start()
    for copy in copies:
        copy.wait()


def swap(value, mesh_shape, partner):
    wide, high = mesh_shape
    moves = []
    for b in range(wide):
        for j in range(high):
            other = partner(b, j)
            if other is not None:
                moves.append((b * high + j, other[0] * high + other[1]))
    return lax.ppermute(value, ("bx", "by"), moves)


def per_device(forcing, guess, shift, ocean):
    rows, cols = forcing.shape
    wide, high = lax.axis_size("bx"), lax.axis_size("by")
    devices = wide * high
    assert rows % SUB == 0 and cols % LANE == 0 and devices % SUB == 0
    assert wide % 2 == 0 and high % 2 == 0
    assert rows % LANE + 2 * SUB <= LANE // 2 and FIELDS * DEPTH <= COLUMNS
    n = FIELDS * SUB
    tall = rows + 2 * SUB
    span = rows // LANE * LANE + LANE
    packed = span // LANE * COLUMNS - SUB
    f32 = functools.partial(jax.ShapeDtypeStruct, dtype=jnp.float32)
    held = functools.partial(pltpu.VMEM, dtype=jnp.float32)
    fields = [pltpu.with_memory_space_constraint(v, pltpu.HBM) for v in (forcing, guess, shift, ocean)]
    edges = [pltpu.VMEM((SUB, cols), v.dtype) for v in fields]
    near, far = call(
        edge_kernel,
        (f32((n, cols)),) * 2,
        [HBM] * 4,
        (VMEM,) * 2,
        edges * 2 + [pltpu.SemaphoreType.DMA((8,))],
    )(*fields)

    def own_chip(b, j):
        return (b, j ^ 1)

    def next_chip(b, j):
        if j == 0:
            return None
        if j == high - 1:
            return (wide - 1 - b, j)
        return (b, ((j - 1) ^ 1) + 1)

    def even_pair(b, j):
        return (b ^ 1, j)

    def odd_pair(b, j):
        return ((((b - 1) % wide) ^ 1) + 1) % wide, j

    shape = (wide, high)
    far = swap(far, shape, next_chip)
    near = swap(near, shape, own_chip)
    x, f, c, columns = call(
        block_kernel,
        (f32((rows, cols)),) * 3 + (f32((2 * COLUMNS, span)),),
        [HBM] * 4,
        (VMEM,) * 4,
        [pltpu.VMEM((rows, cols), v.dtype) for v in fields] + [pltpu.SemaphoreType.DMA((4,))],
    )(*fields)
    halo, a, b = call(
        functools.partial(halo_kernel, rows),
        (f32((2 * n, cols)),) + (f32((packed, LANE)),) * 2,
        [VMEM] * 3,
        (VMEM,) * 3,
    )(far, near, columns)
    a = swap(a, shape, even_pair)
    b = swap(b, shape, odd_pair)
    high = (tall, LANE)
    x, r, pair, *strips = call(
        interior_kernel,
        (held((rows, cols)), held((tall, cols)), held((2 * SUB, LANE))) + (held(high),) * 3,
        [VMEM] * 4,
        (VMEM,) * 6,
        [pltpu.VMEM((tall, cols), jnp.float32)] * 2,
    )(x, f, c, halo)
    strip_x, strip_r, pairs = call(
        strip_kernel,
        (held((rows, LANE)), held(high), held((devices, LANE))),
        [VMEM] * 6,
        (VMEM,) * 3,
        [pltpu.VMEM(high, jnp.float32)] * 2,
    )(*strips, b, a, pair)
    pairs = lax.all_to_all(pairs, ("bx", "by"), 0, 0, tiled=True)
    x, r, norm = call(
        functools.partial(norm_kernel, rows * cols * devices),
        (f32((rows, cols)), f32((rows, cols)), f32((1,))),
        [VMEM] * 5,
        (HBM,) * 3,
        [pltpu.VMEM((rows, cols), jnp.float32)] * 2 + [pltpu.SMEM((1,), jnp.float32), pltpu.SemaphoreType.DMA((3,))],
    )(pairs, x, r, strip_x, strip_r)
    return (x, r, norm[0])


def solution(mesh):
    spec = P("by", "bx")
    return jax.shard_map(
        per_device, mesh=mesh, in_specs=(spec,) * 4, out_specs=(spec, spec, P()), check_vma=False
    )
```

```python
import functools

import jax
import jax.numpy as jnp
from jax import lax
from jax.experimental import pallas as pl
from jax.experimental.pallas import tpu as pltpu
from jax.sharding import PartitionSpec as P

ITERS = 4
LOW_BOUND = 0.05
HIGH_BOUND = 14.5

SUB = 8
LANE = 128
FIELDS = 3
DEPTH = ITERS + 1
COLUMNS = 2 * SUB
LEFT = LANE // 2 - SUB + DEPTH
VMEM = pl.BlockSpec(memory_space=pltpu.VMEM)
HBM = pl.BlockSpec(memory_space=pltpu.HBM)
GRANT = pltpu.CompilerParams(vmem_limit_bytes=8 << 20)


def call(kernel, shapes, in_specs, out_specs, scratch=(), flops=100000):
    return pl.pallas_call(
        kernel,
        out_shape=shapes,
        in_specs=in_specs,
        out_specs=out_specs,
        scratch_shapes=scratch,
        cost_estimate=pl.CostEstimate(flops=flops, bytes_accessed=0, transcendentals=0),
        compiler_params=GRANT,
    )


def masked_fields(forcing, guess, shift, ocean):
    zero = jnp.zeros_like(forcing)
    sea = ocean > 0
    return (
        jnp.where(sea, guess, zero),
        jnp.where(sea, forcing, zero),
        jnp.where(sea, 6.0 + shift, zero),
    )


def is_odd(axis):
    return lax.rem(lax.axis_index(axis), 2) == 1


def edge_kernel(*refs):
    near_ref, far_ref = refs[4:6]
    low_s, top_s = refs[6:10], refs[10:14]
    sem = refs[14]
    rows = refs[0].shape[0]
    copies = []
    for i in range(4):
        copies.append(pltpu.make_async_copy(refs[i].at[0:SUB, :], low_s[i], sem.at[2 * i]))
        copies.append(pltpu.make_async_copy(refs[i].at[rows - SUB : rows, :], top_s[i], sem.at[2 * i + 1]))
    for copy in copies:
        copy.start()
    odd = is_odd("by")
    for copy in copies:
        copy.wait()
    low = masked_fields(*(ref[...] for ref in low_s))
    top = masked_fields(*(ref[...] for ref in top_s))
    for f in range(FIELDS):
        at = slice(f * SUB, (f + 1) * SUB)
        near_ref[at, :] = jnp.where(odd, low[f], top[f])
        far_ref[at, :] = jnp.where(odd, top[f], low[f])


def pack_columns(fields):
    rows, cols = fields[0].shape
    lane = lax.broadcasted_iota(jnp.int32, (rows, LANE), 1)
    packed = jnp.zeros((rows, LANE), jnp.float32)
    for f, field in enumerate(fields):
        at = f * DEPTH
        left = field[:, :LANE]
        left = pltpu.roll(left, at, 1) if at else left
        packed = jnp.where((lane >= at) & (lane < at + DEPTH), left, packed)
        at = COLUMNS + f * DEPTH
        right = pltpu.roll(field[:, cols - LANE :], at + DEPTH, 1)
        packed = jnp.where((lane >= at) & (lane < at + DEPTH), right, packed)
    return packed


def block_kernel(*refs):
    x_ref, r_ref, c_ref, columns_ref = refs[4:8]
    held, sem = refs[8:12], refs[12]
    copies = [pltpu.make_async_copy(refs[i], held[i], sem.at[i]) for i in range(4)]
    for copy in copies:
        copy.start()
    for copy in copies:
        copy.wait()
    fields = masked_fields(*(ref[...] for ref in held))
    for ref, field in zip((x_ref, r_ref, c_ref), fields):
        ref[...] = field
    packed = pack_columns(fields)
    width = columns_ref.shape[1]
    packed = jnp.concatenate([packed, jnp.zeros((width - packed.shape[0], LANE), jnp.float32)], axis=0)
    columns_ref[...] = packed.T[: 2 * COLUMNS]


def mirrored(tile):
    back = LANE - 1 - lax.broadcasted_iota(jnp.int32, (SUB, LANE), 1)
    up = SUB - 1 - lax.broadcasted_iota(jnp.int32, (SUB, LANE), 0)
    parts = []
    for at in reversed(range(0, tile.shape[1], LANE)):
        part = jnp.take_along_axis(tile[:, at : at + LANE], back, axis=1)
        parts.append(jnp.take_along_axis(part, up, axis=0))
    return jnp.concatenate(parts, axis=1)


def halo_kernel(rows, far_ref, near_ref, columns_ref, halo_ref, a_ref, b_ref):
    odd, odd_x = is_odd("by"), is_odd("bx")
    fold = lax.axis_index("by") == lax.axis_size("by") - 1
    n = FIELDS * SUB
    near, far = near_ref[...], far_ref[...]
    halo_ref[0:n, :] = jnp.where(odd, far, near)
    halo_ref[n : 2 * n, :] = jnp.where(lax.axis_index("by") == 0, 0.0, jnp.where(odd, near, far))

    @pl.when(fold)
    def _():
        for f in range(FIELDS):
            at = slice(f * SUB, (f + 1) * SUB)
            halo_ref[at, :] = mirrored(halo_ref[at, :])

    fields = [
        jnp.concatenate([halo_ref[f * SUB : (f + 1) * SUB, :], halo_ref[n + f * SUB : n + (f + 1) * SUB, :]], axis=0)
        for f in range(FIELDS)
    ]
    packed = pack_columns(fields)
    width = columns_ref.shape[1]
    start = width - LANE
    before, after = rows - start, width - rows - 2 * SUB
    pieces = [packed]
    if before:
        pieces.insert(0, jnp.zeros((before, LANE), jnp.float32))
    if after:
        pieces.append(jnp.zeros((after, LANE), jnp.float32))
    rest = columns_ref[:, start:width] + jnp.concatenate(pieces, axis=0).T[: 2 * COLUMNS]
    sides = []
    for at in (slice(0, COLUMNS), slice(COLUMNS, 2 * COLUMNS)):
        parts = [columns_ref[at, p : p + LANE] for p in range(0, start, LANE)]
        sides.append(jnp.concatenate(parts + [folded(rest[at])], axis=0))
    a_ref[...] = jnp.where(odd_x, sides[0], sides[1])
    b_ref[...] = jnp.where(odd_x, sides[1], sides[0])


def folded(rest):
    return rest[0:SUB] + pltpu.roll(rest[SUB:COLUMNS], LANE // 2, 1)


def unfolded(value):
    parts = [value[p : p + COLUMNS] for p in range(0, value.shape[0] - SUB, COLUMNS)]
    rest = value[value.shape[0] - SUB :]
    parts.append(jnp.concatenate([rest, pltpu.roll(rest, LANE // 2, 1)], axis=0))
    return jnp.concatenate(parts, axis=1)


def coefficients():
    theta = (HIGH_BOUND + LOW_BOUND) / 2.0
    delta = (HIGH_BOUND - LOW_BOUND) / 2.0
    sigma = theta / delta
    rho = 1.0 / sigma
    steps = []
    for _ in range(ITERS):
        following = 1.0 / (2.0 * sigma - rho)
        steps.append((following * rho, 2.0 * following / delta))
        rho = following
    return theta, steps


def pair_add(first, second):
    total = first[0] + second[0]
    backed = total - first[0]
    error = (first[0] - (total - backed)) + (second[0] - backed)
    return (total, (first[1] + second[1]) + error)


def settled(pair):
    upper = pair[0] + pair[1]
    return (upper, pair[1] - (upper - pair[0]))


def pair_tree(pairs):
    while len(pairs) > 1:
        tail = pairs[len(pairs) // 2 * 2 :]
        pairs = [pair_add(pairs[i], pairs[i + 1]) for i in range(0, len(pairs) - 1, 2)] + tail
    return pairs[0]


def pair_total(pairs):
    total = pair_tree(pairs)
    for by in (4, 2, 1):
        total = pair_add(total, tuple(pltpu.roll(v, by, 0) for v in total))
    return total


def sweeps(inner, x_s, d_s, r_s, c_s, weigh):
    tall, wide = d_s.shape
    tiles = tall // SUB
    theta, steps = coefficients()
    row_id = lax.broadcasted_iota(jnp.int32, (SUB, wide), 0)
    first_row, last_row = row_id == 0, row_id == SUB - 1

    def across(i):
        v = d_s[i * SUB : (i + 1) * SUB, :]
        pair = pltpu.roll(v, 1, 1) + pltpu.roll(v, wide - 1, 1)
        mixed = v + 0.5 * pair
        return v, pair, pltpu.roll(mixed, 1, 0), pltpu.roll(mixed, SUB - 1, 0)

    squares = []
    for sweep in range(ITERS + 1):
        head, tail = across(0), across(tiles - 1)
        before, now = tail, head
        for i in range(tiles):
            if i < tiles - 2:
                after = across(i + 1)
            else:
                after = tail if i == tiles - 2 else head
            v, pair, down, up = now
            from_below = jnp.where(first_row, before[2], down)
            from_above = jnp.where(last_row, after[3], up)
            at = slice(i * SUB, (i + 1) * SUB)
            c = c_s[at, :]
            image = jnp.where(c > 0.0, c * v - (pair + (from_below + from_above)), jnp.zeros_like(c))
            r = r_s[at, :] - image
            if sweep < ITERS:
                r_s[at, :] = r
                if sweep == 0:
                    d = r * (1.0 / theta)
                else:
                    keep, gain = steps[sweep - 1]
                    d = keep * v + gain * r
                d_s[at, :] = d
                if i < inner:
                    x_s[at, :] = (v if sweep == 0 else x_s[at, :]) + d
            elif i < inner:
                r_s[at, :] = r
                r = jnp.where(weigh, r, jnp.zeros_like(r))
                squares.append(jnp.sum(r * r, axis=1, keepdims=True))
            before, now = now, after
    zero = jnp.zeros_like(squares[0])
    return pair_total([(q, zero) for q in squares])


def interior_kernel(x_ref, f_ref, c_ref, halo_ref, out_x_ref, out_r_ref, pair_ref, strip_x, strip_r, strip_c, d_s, c_s):
    rows, cols = x_ref.shape
    high = d_s.shape[0]
    n = FIELDS * SUB
    lane = lax.broadcasted_iota(jnp.int32, (high, LANE), 1)
    left, right = (lane >= LEFT) & (lane < LEFT + 2 * SUB), lane >= LANE - 2 * SUB
    for f, (ref, main, strip) in enumerate(((d_s, x_ref, strip_x), (out_r_ref, f_ref, strip_r), (c_s, c_ref, strip_c))):
        ref[0:rows, :] = main[...]
        ref[rows : rows + SUB, :] = halo_ref[f * SUB : (f + 1) * SUB, :]
        ref[rows + SUB : high, :] = halo_ref[n + f * SUB : n + (f + 1) * SUB, :]
        ends = jnp.where(left, pltpu.roll(ref[:, 0:LANE], LEFT, 1), 0.0)
        strip[...] = jnp.where(right, ref[:, cols - LANE : cols], ends)
    column = lax.broadcasted_iota(jnp.int32, (SUB, cols), 1)
    weigh = (column >= SUB) & (column < cols - SUB)
    upper, lower = sweeps(rows // SUB, out_x_ref, d_s, out_r_ref, c_s, weigh)
    pair_ref[0:SUB, :] = jnp.broadcast_to(upper, (SUB, LANE))
    pair_ref[SUB : 2 * SUB, :] = jnp.broadcast_to(lower, (SUB, LANE))


def strip_kernel(strip_x, strip_r, strip_c, b_ref, a_ref, pair_ref, out_x_ref, out_r_ref, pairs_ref, d_s, c_s):
    odd_x = is_odd("bx")
    high = d_s.shape[0]
    a, b = unfolded(a_ref[...]), unfolded(b_ref[...])
    left, right = jnp.where(odd_x, a, b), jnp.where(odd_x, b, a)
    start = LEFT - DEPTH
    gap = jnp.zeros((start - COLUMNS, a.shape[1]), jnp.float32)
    rest = jnp.zeros((LANE - start - COLUMNS, a.shape[1]), jnp.float32)
    sides = jnp.concatenate([right, gap, left, rest], axis=0).T[0:high]
    lane = lax.broadcasted_iota(jnp.int32, (high, LANE), 1)
    ghost = (lane < DEPTH) | ((lane >= start) & (lane < LEFT))
    for f, (ref, strip) in enumerate(((d_s, strip_x), (out_r_ref, strip_r), (c_s, strip_c))):
        side = pltpu.roll(sides, LANE - f * DEPTH, 1) if f else sides
        ref[...] = jnp.where(ghost, side, strip[...])
    lane = lax.broadcasted_iota(jnp.int32, (SUB, LANE), 1)
    weigh = ((lane >= LEFT) & (lane < LEFT + SUB)) | (lane >= LANE - SUB)
    ends = sweeps(out_x_ref.shape[0] // SUB, out_x_ref, d_s, out_r_ref, c_s, weigh)
    upper, lower = settled(pair_add(ends, (pair_ref[0:SUB, :], pair_ref[SUB : 2 * SUB, :])))
    tile = jnp.where(lane < LANE // 2, upper, lower)
    for i in range(pairs_ref.shape[0] // SUB):
        pairs_ref[i * SUB : (i + 1) * SUB, :] = tile


def norm_kernel(cells, pairs_ref, x_ref, r_ref, strip_x, strip_r, x_hbm, r_hbm, norm_hbm, x_s, r_s, norm_s, sem):
    rows, cols = x_s.shape
    lane = lax.broadcasted_iota(jnp.int32, (rows, LANE), 1)
    copies = []
    for i, (main, strip, joined, out) in enumerate(((x_ref, strip_x, x_s, x_hbm), (r_ref, strip_r, r_s, r_hbm))):
        joined[...] = main[0:rows, :]
        ends = strip[0:rows, :]
        joined[:, 0:LANE] = jnp.where(lane < SUB, pltpu.roll(ends, LANE - LEFT, 1), joined[:, 0:LANE])
        joined[:, cols - LANE : cols] = jnp.where(lane >= LANE - SUB, ends, joined[:, cols - LANE : cols])
        copies.append(pltpu.make_async_copy(joined, out, sem.at[i]))
        copies[i].start()
    pairs = []
    for i in range(pairs_ref.shape[0] // SUB):
        upper = pairs_ref[i * SUB : (i + 1) * SUB, :]
        pairs.append((upper, pltpu.roll(upper, LANE // 2, 1)))
    upper, lower = settled(pair_total(pairs))
    norm_s[0] = jnp.sqrt((upper + lower) * (1.0 / cells))[0, 0]
    copies.append(pltpu.make_async_copy(norm_s, norm_hbm, sem.at[2]))
    copies[2].start()
    for copy in copies:
        copy.wait()


def swap(value, mesh_shape, partner):
    wide, high = mesh_shape
    moves = []
    for b in range(wide):
        for j in range(high):
            other = partner(b, j)
            if other is not None:
                moves.append((b * high + j, other[0] * high + other[1]))
    return lax.ppermute(value, ("bx", "by"), moves)


def per_device(forcing, guess, shift, ocean):
    rows, cols = forcing.shape
    wide, high = lax.axis_size("bx"), lax.axis_size("by")
    devices = wide * high
    assert rows % SUB == 0 and cols % LANE == 0 and devices % SUB == 0
    assert wide % 2 == 0 and high % 2 == 0
    assert rows % LANE + 2 * SUB <= LANE // 2 and FIELDS * DEPTH <= COLUMNS
    n = FIELDS * SUB
    tall = rows + 2 * SUB
    span = rows // LANE * LANE + LANE
    packed = span // LANE * COLUMNS - SUB
    f32 = functools.partial(jax.ShapeDtypeStruct, dtype=jnp.float32)
    held = functools.partial(pltpu.VMEM, dtype=jnp.float32)
    fields = [pltpu.with_memory_space_constraint(v, pltpu.HBM) for v in (forcing, guess, shift, ocean)]
    edges = [pltpu.VMEM((SUB, cols), v.dtype) for v in fields]
    near, far = call(
        edge_kernel,
        (f32((n, cols)),) * 2,
        [HBM] * 4,
        (VMEM,) * 2,
        edges * 2 + [pltpu.SemaphoreType.DMA((8,))],
    )(*fields)

    def own_chip(b, j):
        return (b, j ^ 1)

    def next_chip(b, j):
        if j == 0:
            return (b ^ 1, j)
        if j == high - 1:
            return (wide - 1 - b, j)
        return (b, ((j - 1) ^ 1) + 1)

    def even_pair(b, j):
        return (b ^ 1, j)

    def odd_pair(b, j):
        return ((((b - 1) % wide) ^ 1) + 1) % wide, j

    shape = (wide, high)
    far = swap(far, shape, next_chip)
    near = swap(near, shape, own_chip)
    x, f, c, columns = call(
        block_kernel,
        (f32((rows, cols)),) * 3 + (f32((2 * COLUMNS, span)),),
        [HBM] * 4,
        (VMEM,) * 4,
        [pltpu.VMEM((rows, cols), v.dtype) for v in fields] + [pltpu.SemaphoreType.DMA((4,))],
    )(*fields)
    halo, a, b = call(
        functools.partial(halo_kernel, rows),
        (f32((2 * n, cols)),) + (f32((packed, LANE)),) * 2,
        [VMEM] * 3,
        (VMEM,) * 3,
    )(far, near, columns)
    a = swap(a, shape, even_pair)
    b = swap(b, shape, odd_pair)
    high = (tall, LANE)
    x, r, pair, *strips = call(
        interior_kernel,
        (held((rows, cols)), held((tall, cols)), held((2 * SUB, LANE))) + (held(high),) * 3,
        [VMEM] * 4,
        (VMEM,) * 6,
        [pltpu.VMEM((tall, cols), jnp.float32)] * 2,
    )(x, f, c, halo)
    strip_x, strip_r, pairs = call(
        strip_kernel,
        (held((rows, LANE)), held(high), held((devices, LANE))),
        [VMEM] * 6,
        (VMEM,) * 3,
        [pltpu.VMEM(high, jnp.float32)] * 2,
    )(*strips, b, a, pair)
    pairs = lax.all_to_all(pairs, ("bx", "by"), 0, 0, tiled=True)
    x, r, norm = call(
        functools.partial(norm_kernel, rows * cols * devices),
        (f32((rows, cols)), f32((rows, cols)), f32((1,))),
        [VMEM] * 5,
        (HBM,) * 3,
        [pltpu.VMEM((rows, cols), jnp.float32)] * 2 + [pltpu.SMEM((1,), jnp.float32), pltpu.SemaphoreType.DMA((3,))],
    )(pairs, x, r, strip_x, strip_r)
    return (x, r, norm[0])


def solution(mesh):
    spec = P("by", "bx")
    return jax.shard_map(
        per_device, mesh=mesh, in_specs=(spec,) * 4, out_specs=(spec, spec, P()), check_vma=False
    )
```

```python
import functools

import jax
import jax.numpy as jnp
from jax import lax
from jax.experimental import pallas as pl
from jax.experimental.pallas import tpu as pltpu
from jax.sharding import PartitionSpec as P

ITERS = 4
LOW_BOUND = 0.05
HIGH_BOUND = 14.5

SUB = 8
LANE = 128
FIELDS = 3
DEPTH = ITERS + 1
COLUMNS = 2 * SUB
LEFT = LANE // 2 - SUB + DEPTH
VMEM = pl.BlockSpec(memory_space=pltpu.VMEM)
HBM = pl.BlockSpec(memory_space=pltpu.HBM)
GRANT = pltpu.CompilerParams(vmem_limit_bytes=8 << 20)


def call(kernel, shapes, in_specs, out_specs, scratch=(), flops=100000):
    return pl.pallas_call(
        kernel,
        out_shape=shapes,
        in_specs=in_specs,
        out_specs=out_specs,
        scratch_shapes=scratch,
        cost_estimate=pl.CostEstimate(flops=flops, bytes_accessed=0, transcendentals=0),
        compiler_params=GRANT,
    )


def masked_fields(forcing, guess, shift, ocean):
    zero = jnp.zeros_like(forcing)
    sea = ocean > 0
    return (
        jnp.where(sea, guess, zero),
        jnp.where(sea, forcing, zero),
        jnp.where(sea, 6.0 + shift, zero),
    )


def is_odd(axis):
    return lax.rem(lax.axis_index(axis), 2) == 1


def edge_kernel(*refs):
    near_ref, far_ref = refs[4:6]
    low_s, top_s = refs[6:10], refs[10:14]
    sem = refs[14]
    rows = refs[0].shape[0]
    copies = []
    for i in range(4):
        copies.append(pltpu.make_async_copy(refs[i].at[0:SUB, :], low_s[i], sem.at[2 * i]))
        copies.append(pltpu.make_async_copy(refs[i].at[rows - SUB : rows, :], top_s[i], sem.at[2 * i + 1]))
    for copy in copies:
        copy.start()
    odd = is_odd("by")
    for copy in copies:
        copy.wait()
    low = masked_fields(*(ref[...] for ref in low_s))
    top = masked_fields(*(ref[...] for ref in top_s))
    for f in range(FIELDS):
        at = slice(f * SUB, (f + 1) * SUB)
        near_ref[at, :] = jnp.where(odd, low[f], top[f])
        far_ref[at, :] = jnp.where(odd, top[f], low[f])


def place(index):
    per = LANE // COLUMNS
    return index // per * SUB, index % per * COLUMNS


def end_columns(fields, lane, index):
    zero = jnp.zeros((SUB, LANE), jnp.float32)
    left, right = zero, zero
    for f, field in enumerate(fields):
        at = place(index)[1] + f * DEPTH
        first, last = field[:, :LANE], field[:, field.shape[1] - LANE :]
        left = jnp.where((lane >= at) & (lane < at + DEPTH), pltpu.roll(first, at, 1) if at else first, left)
        at = (at + LEFT - DEPTH) % LANE
        here = (lane >= at) & (lane < at + DEPTH) | (lane < at + DEPTH - LANE)
        right = jnp.where(here, pltpu.roll(last, (at + DEPTH) % LANE, 1), right)
    return left, right


def block_kernel(*refs):
    x_ref, r_ref, c_ref, columns_ref = refs[4:8]
    held, sem = refs[8:12], refs[12]
    copies = [pltpu.make_async_copy(refs[i], held[i], sem.at[i]) for i in range(4)]
    for copy in copies:
        copy.start()
    for copy in copies:
        copy.wait()
    fields = masked_fields(*(ref[...] for ref in held))
    for ref, field in zip((x_ref, r_ref, c_ref), fields):
        ref[...] = field
    lane = lax.broadcasted_iota(jnp.int32, (SUB, LANE), 1)
    half = columns_ref.shape[0] // 2
    sums = {}
    for t in range(x_ref.shape[0] // SUB):
        ends = end_columns([field[t * SUB : (t + 1) * SUB] for field in fields], lane, t)
        row = place(t)[0]
        sums[row] = [p + q for p, q in zip(sums[row], ends)] if row in sums else ends
    for row in range(0, half, SUB):
        left, right = sums.get(row, [jnp.zeros((SUB, LANE), jnp.float32)] * 2)
        columns_ref[row : row + SUB, :] = left
        columns_ref[half + row : half + row + SUB, :] = right


def mirrored(tile):
    back = LANE - 1 - lax.broadcasted_iota(jnp.int32, (SUB, LANE), 1)
    up = SUB - 1 - lax.broadcasted_iota(jnp.int32, (SUB, LANE), 0)
    parts = []
    for at in reversed(range(0, tile.shape[1], LANE)):
        part = jnp.take_along_axis(tile[:, at : at + LANE], back, axis=1)
        parts.append(jnp.take_along_axis(part, up, axis=0))
    return jnp.concatenate(parts, axis=1)


def halo_kernel(rows, far_ref, near_ref, columns_ref, halo_ref, a_ref, b_ref):
    odd, odd_x = is_odd("by"), is_odd("bx")
    fold = lax.axis_index("by") == lax.axis_size("by") - 1
    n = FIELDS * SUB
    near, far = near_ref[...], far_ref[...]
    halo_ref[0:n, :] = jnp.where(odd, far, near)
    halo_ref[n : 2 * n, :] = jnp.where(lax.axis_index("by") == 0, 0.0, jnp.where(odd, near, far))

    @pl.when(fold)
    def _():
        for f in range(FIELDS):
            at = slice(f * SUB, (f + 1) * SUB)
            halo_ref[at, :] = mirrored(halo_ref[at, :])

    lane = lax.broadcasted_iota(jnp.int32, (SUB, LANE), 1)
    half = a_ref.shape[0]
    left = [columns_ref[p : p + SUB, :] for p in range(0, half, SUB)]
    right = [columns_ref[half + p : half + p + SUB, :] for p in range(0, half, SUB)]
    for i in range(2):
        fields = [halo_ref[i * n + f * SUB : i * n + (f + 1) * SUB, :] for f in range(FIELDS)]
        first, last = end_columns(fields, lane, rows // SUB + i)
        g = place(rows // SUB + i)[0] // SUB
        left[g], right[g] = left[g] + first, right[g] + last
    for g in range(half // SUB):
        at = slice(g * SUB, (g + 1) * SUB)
        a_ref[at, :] = jnp.where(odd_x, left[g], right[g])
        b_ref[at, :] = jnp.where(odd_x, right[g], left[g])


def coefficients():
    theta = (HIGH_BOUND + LOW_BOUND) / 2.0
    delta = (HIGH_BOUND - LOW_BOUND) / 2.0
    sigma = theta / delta
    rho = 1.0 / sigma
    steps = []
    for _ in range(ITERS):
        following = 1.0 / (2.0 * sigma - rho)
        steps.append((following * rho, 2.0 * following / delta))
        rho = following
    return theta, steps


def pair_add(first, second):
    total = first[0] + second[0]
    backed = total - first[0]
    error = (first[0] - (total - backed)) + (second[0] - backed)
    return (total, (first[1] + second[1]) + error)


def settled(pair):
    upper = pair[0] + pair[1]
    return (upper, pair[1] - (upper - pair[0]))


def pair_tree(pairs):
    while len(pairs) > 1:
        tail = pairs[len(pairs) // 2 * 2 :]
        pairs = [pair_add(pairs[i], pairs[i + 1]) for i in range(0, len(pairs) - 1, 2)] + tail
    return pairs[0]


def pair_total(pairs):
    total = pair_tree(pairs)
    for by in (4, 2, 1):
        total = pair_add(total, tuple(pltpu.roll(v, by, 0) for v in total))
    return total


def sweeps(inner, x_s, d_s, r_s, c_s, weigh):
    tall, wide = d_s.shape
    tiles = tall // SUB
    theta, steps = coefficients()
    row_id = lax.broadcasted_iota(jnp.int32, (SUB, wide), 0)
    first_row, last_row = row_id == 0, row_id == SUB - 1

    def across(i):
        v = d_s[i * SUB : (i + 1) * SUB, :]
        pair = pltpu.roll(v, 1, 1) + pltpu.roll(v, wide - 1, 1)
        mixed = v + 0.5 * pair
        return v, pair, pltpu.roll(mixed, 1, 0), pltpu.roll(mixed, SUB - 1, 0)

    squares = []
    for sweep in range(ITERS + 1):
        head, tail = across(0), across(tiles - 1)
        before, now = tail, head
        for i in range(tiles):
            if i < tiles - 2:
                after = across(i + 1)
            else:
                after = tail if i == tiles - 2 else head
            v, pair, down, up = now
            from_below = jnp.where(first_row, before[2], down)
            from_above = jnp.where(last_row, after[3], up)
            at = slice(i * SUB, (i + 1) * SUB)
            c = c_s[at, :]
            image = jnp.where(c > 0.0, c * v - (pair + (from_below + from_above)), jnp.zeros_like(c))
            r = r_s[at, :] - image
            if sweep < ITERS:
                r_s[at, :] = r
                if sweep == 0:
                    d = r * (1.0 / theta)
                else:
                    keep, gain = steps[sweep - 1]
                    d = keep * v + gain * r
                d_s[at, :] = d
                if i < inner:
                    x_s[at, :] = (v if sweep == 0 else x_s[at, :]) + d
            elif i < inner:
                r_s[at, :] = r
                r = jnp.where(weigh, r, jnp.zeros_like(r))
                squares.append(jnp.sum(r * r, axis=1, keepdims=True))
            before, now = now, after
    zero = jnp.zeros_like(squares[0])
    return pair_total([(q, zero) for q in squares])


def staggered(inner, x_s, d_s, r_s, c_s, weigh, lag):
    tall, wide = d_s.shape
    tiles = tall // SUB
    theta, steps = coefficients()
    row_id = lax.broadcasted_iota(jnp.int32, (SUB, wide), 0)
    first_row, last_row = row_id == 0, row_id == SUB - 1
    order = [tiles - 1] + list(range(tiles - 1))

    def across(v):
        pair = pltpu.roll(v, 1, 1) + pltpu.roll(v, wide - 1, 1)
        mixed = v + 0.5 * pair
        return v, pair, pltpu.roll(mixed, 1, 0), pltpu.roll(mixed, SUB - 1, 0)

    squares = []
    held = [{} for _ in range(ITERS + 1)]
    for step in range(tiles + 1 + lag * ITERS):
        if step < tiles:
            at = order[step] * SUB
            held[0][step] = across(d_s[at : at + SUB, :])
        for sweep in range(ITERS + 1):
            p = step - 1 - lag * sweep
            if not 0 <= p < tiles:
                continue
            v, pair, down, up = held[sweep][p]
            before, after = held[sweep].pop(p - 1, None), held[sweep].get(p + 1)
            main = order[p] < inner
            if sweep == ITERS and not main:
                continue
            from_below = down if before is None else jnp.where(first_row, before[2], down)
            from_above = up if after is None else jnp.where(last_row, after[3], up)
            at = slice(order[p] * SUB, (order[p] + 1) * SUB)
            c = c_s[at, :]
            image = jnp.where(c > 0.0, c * v - (pair + (from_below + from_above)), jnp.zeros_like(c))
            r = r_s[at, :] - image
            r_s[at, :] = r
            if sweep < ITERS:
                if sweep == 0:
                    d = r * (1.0 / theta)
                else:
                    keep, gain = steps[sweep - 1]
                    d = keep * v + gain * r
                held[sweep + 1][p] = across(d)
                if main:
                    x_s[at, :] = (v if sweep == 0 else x_s[at, :]) + d
            else:
                r = jnp.where(weigh, r, jnp.zeros_like(r))
                squares.append(jnp.sum(r * r, axis=1, keepdims=True))
    zero = jnp.zeros_like(squares[0])
    return pair_total([(q, zero) for q in squares])


def interior_kernel(x_ref, f_ref, c_ref, halo_ref, out_x_ref, out_r_ref, pair_ref, strip_x, strip_r, strip_c, d_s, c_s):
    rows, cols = x_ref.shape
    high = d_s.shape[0]
    n = FIELDS * SUB
    lane = lax.broadcasted_iota(jnp.int32, (high, LANE), 1)
    left, right = (lane >= LEFT) & (lane < LEFT + 2 * SUB), lane >= LANE - 2 * SUB
    for f, (ref, main, strip) in enumerate(((d_s, x_ref, strip_x), (out_r_ref, f_ref, strip_r), (c_s, c_ref, strip_c))):
        ref[0:rows, :] = main[...]
        ref[rows : rows + SUB, :] = halo_ref[f * SUB : (f + 1) * SUB, :]
        ref[rows + SUB : high, :] = halo_ref[n + f * SUB : n + (f + 1) * SUB, :]
        ends = jnp.where(left, pltpu.roll(ref[:, 0:LANE], LEFT, 1), 0.0)
        strip[...] = jnp.where(right, ref[:, cols - LANE : cols], ends)
    column = lax.broadcasted_iota(jnp.int32, (SUB, cols), 1)
    weigh = (column >= SUB) & (column < cols - SUB)
    upper, lower = sweeps(rows // SUB, out_x_ref, d_s, out_r_ref, c_s, weigh)
    pair_ref[0:SUB, :] = jnp.broadcast_to(upper, (SUB, LANE))
    pair_ref[SUB : 2 * SUB, :] = jnp.broadcast_to(lower, (SUB, LANE))


def strip_kernel(strip_x, strip_r, strip_c, b_ref, a_ref, pair_ref, out_x_ref, out_r_ref, pairs_ref, d_s, c_s):
    odd_x = is_odd("bx")
    high = d_s.shape[0]
    a, b = a_ref[...], b_ref[...]
    left, right = jnp.where(odd_x, a, b), jnp.where(odd_x, b, a)
    start = LEFT - DEPTH
    lane = lax.broadcasted_iota(jnp.int32, (SUB, LANE), 1)
    ghost = ((lane >= start) & (lane < LEFT)) | (lane < DEPTH)
    fields = ((d_s, strip_x), (out_r_ref, strip_r), (c_s, strip_c))
    for t in range(high // SUB):
        row, at = place(t)
        rows = slice(t * SUB, (t + 1) * SUB)
        both = jnp.where((lane >= at) & (lane < at + COLUMNS), right[row : row + SUB], left[row : row + SUB])
        for f, (ref, strip) in enumerate(fields):
            by = (LANE - at - f * DEPTH) % LANE
            ref[rows, :] = jnp.where(ghost, pltpu.roll(both, by, 1) if by else both, strip[rows, :])
    lane = lax.broadcasted_iota(jnp.int32, (SUB, LANE), 1)
    weigh = ((lane >= LEFT) & (lane < LEFT + SUB)) | (lane >= LANE - SUB)
    ends = staggered(out_x_ref.shape[0] // SUB, out_x_ref, d_s, out_r_ref, c_s, weigh, 3)
    upper, lower = settled(pair_add(ends, (pair_ref[0:SUB, :], pair_ref[SUB : 2 * SUB, :])))
    tile = jnp.where(lane < LANE // 2, upper, lower)
    for i in range(pairs_ref.shape[0] // SUB):
        pairs_ref[i * SUB : (i + 1) * SUB, :] = tile


def norm_kernel(cells, pairs_ref, x_ref, r_ref, strip_x, strip_r, x_hbm, r_hbm, norm_hbm, x_s, r_s, norm_s, sem):
    rows, cols = x_s.shape
    lane = lax.broadcasted_iota(jnp.int32, (rows, LANE), 1)
    copies = []
    for i, (main, strip, joined, out) in enumerate(((x_ref, strip_x, x_s, x_hbm), (r_ref, strip_r, r_s, r_hbm))):
        joined[...] = main[0:rows, :]
        ends = strip[0:rows, :]
        joined[:, 0:LANE] = jnp.where(lane < SUB, pltpu.roll(ends, LANE - LEFT, 1), joined[:, 0:LANE])
        joined[:, cols - LANE : cols] = jnp.where(lane >= LANE - SUB, ends, joined[:, cols - LANE : cols])
        copies.append(pltpu.make_async_copy(joined, out, sem.at[i]))
        copies[i].start()
    pairs = []
    for i in range(pairs_ref.shape[0] // SUB):
        upper = pairs_ref[i * SUB : (i + 1) * SUB, :]
        pairs.append((upper, pltpu.roll(upper, LANE // 2, 1)))
    upper, lower = settled(pair_total(pairs))
    norm_s[...] = jnp.sqrt((upper + lower) * (1.0 / cells))[0, 0:1]
    copies.append(pltpu.make_async_copy(norm_s, norm_hbm, sem.at[2]))
    copies[2].start()
    for copy in copies:
        copy.wait()


def swap(value, mesh_shape, partner):
    wide, high = mesh_shape
    moves = []
    for b in range(wide):
        for j in range(high):
            other = partner(b, j)
            if other is not None:
                moves.append((b * high + j, other[0] * high + other[1]))
    return lax.ppermute(value, ("bx", "by"), moves)


def per_device(forcing, guess, shift, ocean):
    rows, cols = forcing.shape
    wide, high = lax.axis_size("bx"), lax.axis_size("by")
    devices = wide * high
    assert rows % SUB == 0 and cols % LANE == 0 and devices % SUB == 0
    assert wide % 2 == 0 and high % 2 == 0
    assert FIELDS * DEPTH <= COLUMNS
    n = FIELDS * SUB
    tall = rows + 2 * SUB
    packed = -(-tall // (SUB * (LANE // COLUMNS))) * SUB
    f32 = functools.partial(jax.ShapeDtypeStruct, dtype=jnp.float32)
    held = functools.partial(pltpu.VMEM, dtype=jnp.float32)
    fields = [pltpu.with_memory_space_constraint(v, pltpu.HBM) for v in (forcing, guess, shift, ocean)]
    edges = [pltpu.VMEM((SUB, cols), v.dtype) for v in fields]
    near, far = call(
        edge_kernel,
        (f32((n, cols)),) * 2,
        [HBM] * 4,
        (VMEM,) * 2,
        edges * 2 + [pltpu.SemaphoreType.DMA((8,))],
    )(*fields)

    def own_chip(b, j):
        return (b, j ^ 1)

    def next_chip(b, j):
        if j == 0:
            return (wide - 1 - b, j)
        if j == high - 1:
            return (wide - 1 - b, j)
        return (b, ((j - 1) ^ 1) + 1)

    def even_pair(b, j):
        return (b ^ 1, j)

    def odd_pair(b, j):
        return ((((b - 1) % wide) ^ 1) + 1) % wide, j

    shape = (wide, high)
    far = swap(far, shape, next_chip)
    near = swap(near, shape, own_chip)
    x, f, c, columns = call(
        block_kernel,
        (f32((rows, cols)),) * 3 + (f32((2 * packed, LANE)),),
        [HBM] * 4,
        (VMEM,) * 4,
        [pltpu.VMEM((rows, cols), v.dtype) for v in fields] + [pltpu.SemaphoreType.DMA((4,))],
    )(*fields)
    halo, a, b = call(
        functools.partial(halo_kernel, rows),
        (f32((2 * n, cols)),) + (f32((packed, LANE)),) * 2,
        [VMEM] * 3,
        (VMEM,) * 3,
    )(far, near, columns)
    a = swap(a, shape, even_pair)
    b = swap(b, shape, odd_pair)
    high = (tall, LANE)
    x, r, pair, *strips = call(
        interior_kernel,
        (held((rows, cols)), held((tall, cols)), held((2 * SUB, LANE))) + (held(high),) * 3,
        [VMEM] * 4,
        (VMEM,) * 6,
        [pltpu.VMEM((tall, cols), jnp.float32)] * 2,
    )(x, f, c, halo)
    strip_x, strip_r, pairs = call(
        strip_kernel,
        (held((rows, LANE)), held(high), held((devices, LANE))),
        [VMEM] * 6,
        (VMEM,) * 3,
        [pltpu.VMEM(high, jnp.float32)] * 2,
    )(*strips, b, a, pair)
    pairs = lax.all_to_all(pairs, ("bx", "by"), 0, 0, tiled=True)
    x, r, norm = call(
        functools.partial(norm_kernel, rows * cols * devices),
        (f32((rows, cols)), f32((rows, cols)), f32((1,))),
        [VMEM] * 5,
        (HBM,) * 3,
        [pltpu.VMEM((rows, cols), jnp.float32)] * 2 + [pltpu.VMEM((1,), jnp.float32), pltpu.SemaphoreType.DMA((3,))],
    )(pairs, x, r, strip_x, strip_r)
    return (x, r, norm[0])


def solution(mesh):
    spec = P("by", "bx")
    return jax.shard_map(
        per_device, mesh=mesh, in_specs=(spec,) * 4, out_specs=(spec, spec, P()), check_vma=False
    )
```

```python
import functools

import jax
import jax.numpy as jnp
from jax import lax
from jax.experimental import pallas as pl
from jax.experimental.pallas import tpu as pltpu
from jax.sharding import PartitionSpec as P

ITERS = 4
LOW_BOUND = 0.05
HIGH_BOUND = 14.5

SUB = 8
LANE = 128
FIELDS = 3
DEPTH = ITERS + 1
COLUMNS = 2 * SUB
LEFT = LANE // 2 - SUB + DEPTH
VMEM = pl.BlockSpec(memory_space=pltpu.VMEM)
HBM = pl.BlockSpec(memory_space=pltpu.HBM)
GRANT = pltpu.CompilerParams(vmem_limit_bytes=8 << 20)


def call(kernel, shapes, in_specs, out_specs, scratch=(), flops=100000):
    return pl.pallas_call(
        kernel,
        out_shape=shapes,
        in_specs=in_specs,
        out_specs=out_specs,
        scratch_shapes=scratch,
        cost_estimate=pl.CostEstimate(flops=flops, bytes_accessed=0, transcendentals=0),
        compiler_params=GRANT,
    )


def masked_fields(forcing, guess, shift, ocean):
    zero = jnp.zeros_like(forcing)
    sea = ocean > 0
    return (
        jnp.where(sea, guess, zero),
        jnp.where(sea, forcing, zero),
        jnp.where(sea, 6.0 + shift, zero),
    )


def is_odd(axis):
    return lax.rem(lax.axis_index(axis), 2) == 1


def edge_kernel(*refs):
    near_ref, far_ref = refs[4:6]
    low_s, top_s = refs[6:10], refs[10:14]
    sem = refs[14]
    rows = refs[0].shape[0]
    copies = []
    for i in range(4):
        copies.append(pltpu.make_async_copy(refs[i].at[0:SUB, :], low_s[i], sem.at[2 * i]))
        copies.append(pltpu.make_async_copy(refs[i].at[rows - SUB : rows, :], top_s[i], sem.at[2 * i + 1]))
    for copy in copies:
        copy.start()
    odd = is_odd("by")
    for copy in copies:
        copy.wait()
    low = masked_fields(*(ref[...] for ref in low_s))
    top = masked_fields(*(ref[...] for ref in top_s))
    for f in range(FIELDS):
        at = slice(f * SUB, (f + 1) * SUB)
        near_ref[at, :] = jnp.where(odd, low[f], top[f])
        far_ref[at, :] = jnp.where(odd, top[f], low[f])


def place(index):
    per = LANE // COLUMNS
    return index // per * SUB, index % per * COLUMNS


def end_columns(fields, lane, index):
    zero = jnp.zeros((SUB, LANE), jnp.float32)
    left, right = zero, zero
    for f, field in enumerate(fields):
        at = place(index)[1] + f * DEPTH
        first, last = field[:, :LANE], field[:, field.shape[1] - LANE :]
        left = jnp.where((lane >= at) & (lane < at + DEPTH), pltpu.roll(first, at, 1) if at else first, left)
        at = (at + LEFT - DEPTH) % LANE
        here = (lane >= at) & (lane < at + DEPTH) | (lane < at + DEPTH - LANE)
        right = jnp.where(here, pltpu.roll(last, (at + DEPTH) % LANE, 1), right)
    return left, right


def block_kernel(*refs):
    x_ref, r_ref, c_ref, columns_ref = refs[4:8]
    held, sem = refs[8:12], refs[12]
    copies = [pltpu.make_async_copy(refs[i], held[i], sem.at[i]) for i in range(4)]
    for copy in copies:
        copy.start()
    for copy in copies:
        copy.wait()
    fields = masked_fields(*(ref[...] for ref in held))
    for ref, field in zip((x_ref, r_ref, c_ref), fields):
        ref[...] = field
    lane = lax.broadcasted_iota(jnp.int32, (SUB, LANE), 1)
    half = columns_ref.shape[0] // 2
    sums = {}
    for t in range(x_ref.shape[0] // SUB):
        ends = end_columns([field[t * SUB : (t + 1) * SUB] for field in fields], lane, t)
        row = place(t)[0]
        sums[row] = [p + q for p, q in zip(sums[row], ends)] if row in sums else ends
    for row in range(0, half, SUB):
        left, right = sums.get(row, [jnp.zeros((SUB, LANE), jnp.float32)] * 2)
        columns_ref[row : row + SUB, :] = left
        columns_ref[half + row : half + row + SUB, :] = right


def mirrored(tile):
    back = LANE - 1 - lax.broadcasted_iota(jnp.int32, (SUB, LANE), 1)
    up = SUB - 1 - lax.broadcasted_iota(jnp.int32, (SUB, LANE), 0)
    parts = []
    for at in reversed(range(0, tile.shape[1], LANE)):
        part = jnp.take_along_axis(tile[:, at : at + LANE], back, axis=1)
        parts.append(jnp.take_along_axis(part, up, axis=0))
    return jnp.concatenate(parts, axis=1)


def halo_kernel(rows, far_ref, near_ref, columns_ref, halo_ref, a_ref, b_ref):
    odd, odd_x = is_odd("by"), is_odd("bx")
    fold = lax.axis_index("by") == lax.axis_size("by") - 1
    n = FIELDS * SUB
    near, far = near_ref[...], far_ref[...]
    halo_ref[0:n, :] = jnp.where(odd, far, near)
    halo_ref[n : 2 * n, :] = jnp.where(lax.axis_index("by") == 0, 0.0, jnp.where(odd, near, far))

    @pl.when(fold)
    def _():
        for f in range(FIELDS):
            at = slice(f * SUB, (f + 1) * SUB)
            halo_ref[at, :] = mirrored(halo_ref[at, :])

    lane = lax.broadcasted_iota(jnp.int32, (SUB, LANE), 1)
    half = a_ref.shape[0]
    left = [columns_ref[p : p + SUB, :] for p in range(0, half, SUB)]
    right = [columns_ref[half + p : half + p + SUB, :] for p in range(0, half, SUB)]
    for i in range(2):
        fields = [halo_ref[i * n + f * SUB : i * n + (f + 1) * SUB, :] for f in range(FIELDS)]
        first, last = end_columns(fields, lane, rows // SUB + i)
        g = place(rows // SUB + i)[0] // SUB
        left[g], right[g] = left[g] + first, right[g] + last
    for g in range(half // SUB):
        at = slice(g * SUB, (g + 1) * SUB)
        a_ref[at, :] = jnp.where(odd_x, left[g], right[g])
        b_ref[at, :] = jnp.where(odd_x, right[g], left[g])


def coefficients():
    theta = (HIGH_BOUND + LOW_BOUND) / 2.0
    delta = (HIGH_BOUND - LOW_BOUND) / 2.0
    sigma = theta / delta
    rho = 1.0 / sigma
    steps = []
    for _ in range(ITERS):
        following = 1.0 / (2.0 * sigma - rho)
        steps.append((following * rho, 2.0 * following / delta))
        rho = following
    return theta, steps


def pair_add(first, second):
    total = first[0] + second[0]
    backed = total - first[0]
    error = (first[0] - (total - backed)) + (second[0] - backed)
    return (total, (first[1] + second[1]) + error)


def settled(pair):
    upper = pair[0] + pair[1]
    return (upper, pair[1] - (upper - pair[0]))


def pair_tree(pairs):
    while len(pairs) > 1:
        tail = pairs[len(pairs) // 2 * 2 :]
        pairs = [pair_add(pairs[i], pairs[i + 1]) for i in range(0, len(pairs) - 1, 2)] + tail
    return pairs[0]


def pair_total(pairs):
    total = pair_tree(pairs)
    for by in (4, 2, 1):
        total = pair_add(total, tuple(pltpu.roll(v, by, 0) for v in total))
    return total


def sweeps(inner, x_s, d_s, r_s, c_s, weigh):
    tall, wide = d_s.shape
    tiles = tall // SUB
    theta, steps = coefficients()
    row_id = lax.broadcasted_iota(jnp.int32, (SUB, wide), 0)
    first_row, last_row = row_id == 0, row_id == SUB - 1

    def across(i):
        v = d_s[i * SUB : (i + 1) * SUB, :]
        pair = pltpu.roll(v, 1, 1) + pltpu.roll(v, wide - 1, 1)
        mixed = v + 0.5 * pair
        return v, pair, pltpu.roll(mixed, 1, 0), pltpu.roll(mixed, SUB - 1, 0)

    squares = []
    for sweep in range(ITERS + 1):
        head, tail = across(0), across(tiles - 1)
        before, now = tail, head
        for i in range(tiles):
            if i < tiles - 2:
                after = across(i + 1)
            else:
                after = tail if i == tiles - 2 else head
            v, pair, down, up = now
            from_below = jnp.where(first_row, before[2], down)
            from_above = jnp.where(last_row, after[3], up)
            at = slice(i * SUB, (i + 1) * SUB)
            c = c_s[at, :]
            image = jnp.where(c > 0.0, c * v - (pair + (from_below + from_above)), jnp.zeros_like(c))
            r = r_s[at, :] - image
            if sweep < ITERS:
                r_s[at, :] = r
                if sweep == 0:
                    d = r * (1.0 / theta)
                else:
                    keep, gain = steps[sweep - 1]
                    d = keep * v + gain * r
                d_s[at, :] = d
                if i < inner:
                    x_s[at, :] = (v if sweep == 0 else x_s[at, :]) + d
            elif i < inner:
                r_s[at, :] = r
                r = jnp.where(weigh, r, jnp.zeros_like(r))
                squares.append(jnp.sum(r * r, axis=1, keepdims=True))
            before, now = now, after
    zero = jnp.zeros_like(squares[0])
    return pair_total([(q, zero) for q in squares])


def staggered(inner, fill, x_s, r_s, c_s, weigh, lag):
    tall, wide = c_s.shape
    tiles = tall // SUB
    theta, steps = coefficients()
    row_id = lax.broadcasted_iota(jnp.int32, (SUB, wide), 0)
    first_row, last_row = row_id == 0, row_id == SUB - 1
    order = [tiles - 1] + list(range(tiles - 1))

    def across(v):
        pair = pltpu.roll(v, 1, 1) + pltpu.roll(v, wide - 1, 1)
        mixed = v + 0.5 * pair
        return v, pair, pltpu.roll(mixed, 1, 0), pltpu.roll(mixed, SUB - 1, 0)

    squares = []
    held = [{} for _ in range(ITERS + 1)]
    for step in range(tiles + 1 + lag * ITERS):
        if step < tiles:
            held[0][step] = across(fill(order[step]))
        for sweep in range(ITERS + 1):
            p = step - 1 - lag * sweep
            if not 0 <= p < tiles:
                continue
            v, pair, down, up = held[sweep][p]
            before, after = held[sweep].pop(p - 1, None), held[sweep].get(p + 1)
            main = order[p] < inner
            if sweep == ITERS and not main:
                continue
            from_below = down if before is None else jnp.where(first_row, before[2], down)
            from_above = up if after is None else jnp.where(last_row, after[3], up)
            at = slice(order[p] * SUB, (order[p] + 1) * SUB)
            c = c_s[at, :]
            image = jnp.where(c > 0.0, c * v - (pair + (from_below + from_above)), jnp.zeros_like(c))
            r = r_s[at, :] - image
            r_s[at, :] = r
            if sweep < ITERS:
                if sweep == 0:
                    d = r * (1.0 / theta)
                else:
                    keep, gain = steps[sweep - 1]
                    d = keep * v + gain * r
                held[sweep + 1][p] = across(d)
                if main:
                    x_s[at, :] = (v if sweep == 0 else x_s[at, :]) + d
            else:
                r = jnp.where(weigh, r, jnp.zeros_like(r))
                squares.append(jnp.sum(r * r, axis=1, keepdims=True))
    zero = jnp.zeros_like(squares[0])
    return pair_total([(q, zero) for q in squares])


def interior_kernel(x_ref, f_ref, c_ref, halo_ref, out_x_ref, out_r_ref, pair_ref, strip_x, strip_r, strip_c, d_s, c_s):
    rows, cols = x_ref.shape
    high = d_s.shape[0]
    n = FIELDS * SUB
    lane = lax.broadcasted_iota(jnp.int32, (high, LANE), 1)
    left, right = (lane >= LEFT) & (lane < LEFT + 2 * SUB), lane >= LANE - 2 * SUB
    for f, (ref, main, strip) in enumerate(((d_s, x_ref, strip_x), (out_r_ref, f_ref, strip_r), (c_s, c_ref, strip_c))):
        ref[0:rows, :] = main[...]
        ref[rows : rows + SUB, :] = halo_ref[f * SUB : (f + 1) * SUB, :]
        ref[rows + SUB : high, :] = halo_ref[n + f * SUB : n + (f + 1) * SUB, :]
        ends = jnp.where(left, pltpu.roll(ref[:, 0:LANE], LEFT, 1), 0.0)
        strip[...] = jnp.where(right, ref[:, cols - LANE : cols], ends)
    column = lax.broadcasted_iota(jnp.int32, (SUB, cols), 1)
    weigh = (column >= SUB) & (column < cols - SUB)
    upper, lower = sweeps(rows // SUB, out_x_ref, d_s, out_r_ref, c_s, weigh)
    pair_ref[0:SUB, :] = jnp.broadcast_to(upper, (SUB, LANE))
    pair_ref[SUB : 2 * SUB, :] = jnp.broadcast_to(lower, (SUB, LANE))


def strip_kernel(strip_x, strip_r, strip_c, b_ref, a_ref, pair_ref, out_x_ref, out_r_ref, pairs_ref, c_s):
    odd_x = is_odd("bx")
    a, b = a_ref[...], b_ref[...]
    left, right = jnp.where(odd_x, a, b), jnp.where(odd_x, b, a)
    start = LEFT - DEPTH
    lane = lax.broadcasted_iota(jnp.int32, (SUB, LANE), 1)
    ghost = ((lane >= start) & (lane < LEFT)) | (lane < DEPTH)

    def fill(t):
        row, at = place(t)
        rows = slice(t * SUB, (t + 1) * SUB)
        both = jnp.where((lane >= at) & (lane < at + COLUMNS), right[row : row + SUB], left[row : row + SUB])
        values = []
        for f, strip in enumerate((strip_x, strip_r, strip_c)):
            by = (LANE - at - f * DEPTH) % LANE
            values.append(jnp.where(ghost, pltpu.roll(both, by, 1) if by else both, strip[rows, :]))
        out_r_ref[rows, :], c_s[rows, :] = values[1:]
        return values[0]

    lane = lax.broadcasted_iota(jnp.int32, (SUB, LANE), 1)
    weigh = ((lane >= LEFT) & (lane < LEFT + SUB)) | (lane >= LANE - SUB)
    ends = staggered(out_x_ref.shape[0] // SUB, fill, out_x_ref, out_r_ref, c_s, weigh, 3)
    upper, lower = settled(pair_add(ends, (pair_ref[0:SUB, :], pair_ref[SUB : 2 * SUB, :])))
    tile = jnp.where(lane < LANE // 2, upper, lower)
    for i in range(pairs_ref.shape[0] // SUB):
        pairs_ref[i * SUB : (i + 1) * SUB, :] = tile


def norm_kernel(cells, pairs_ref, x_ref, r_ref, strip_x, strip_r, x_hbm, r_hbm, norm_hbm, x_s, r_s, norm_s, sem):
    rows, cols = x_s.shape
    lane = lax.broadcasted_iota(jnp.int32, (rows, LANE), 1)
    copies = []
    for i, (main, strip, joined, out) in enumerate(((x_ref, strip_x, x_s, x_hbm), (r_ref, strip_r, r_s, r_hbm))):
        joined[...] = main[0:rows, :]
        ends = strip[0:rows, :]
        joined[:, 0:LANE] = jnp.where(lane < SUB, pltpu.roll(ends, LANE - LEFT, 1), joined[:, 0:LANE])
        joined[:, cols - LANE : cols] = jnp.where(lane >= LANE - SUB, ends, joined[:, cols - LANE : cols])
        copies.append(pltpu.make_async_copy(joined, out, sem.at[i]))
        copies[i].start()
    pairs = []
    for i in range(pairs_ref.shape[0] // SUB):
        upper = pairs_ref[i * SUB : (i + 1) * SUB, :]
        pairs.append((upper, pltpu.roll(upper, LANE // 2, 1)))
    upper, lower = settled(pair_total(pairs))
    norm_s[...] = jnp.sqrt((upper + lower) * (1.0 / cells))[0, 0:1]
    copies.append(pltpu.make_async_copy(norm_s, norm_hbm, sem.at[2]))
    copies[2].start()
    for copy in copies:
        copy.wait()


def swap(value, mesh_shape, partner):
    wide, high = mesh_shape
    moves = []
    for b in range(wide):
        for j in range(high):
            other = partner(b, j)
            if other is not None:
                moves.append((b * high + j, other[0] * high + other[1]))
    return lax.ppermute(value, ("bx", "by"), moves)


def per_device(forcing, guess, shift, ocean):
    rows, cols = forcing.shape
    wide, high = lax.axis_size("bx"), lax.axis_size("by")
    devices = wide * high
    assert rows % SUB == 0 and cols % LANE == 0 and devices % SUB == 0
    assert wide % 2 == 0 and high % 2 == 0
    assert FIELDS * DEPTH <= COLUMNS
    n = FIELDS * SUB
    tall = rows + 2 * SUB
    packed = -(-tall // (SUB * (LANE // COLUMNS))) * SUB
    f32 = functools.partial(jax.ShapeDtypeStruct, dtype=jnp.float32)
    held = functools.partial(pltpu.VMEM, dtype=jnp.float32)
    fields = [pltpu.with_memory_space_constraint(v, pltpu.HBM) for v in (forcing, guess, shift, ocean)]
    edges = [pltpu.VMEM((SUB, cols), v.dtype) for v in fields]
    near, far = call(
        edge_kernel,
        (f32((n, cols)),) * 2,
        [HBM] * 4,
        (VMEM,) * 2,
        edges * 2 + [pltpu.SemaphoreType.DMA((8,))],
    )(*fields)

    def own_chip(b, j):
        return (b, j ^ 1)

    def next_chip(b, j):
        if j == 0:
            return (wide - 1 - b, j)
        if j == high - 1:
            return (wide - 1 - b, j)
        return (b, ((j - 1) ^ 1) + 1)

    def even_pair(b, j):
        return (b ^ 1, j)

    def odd_pair(b, j):
        return ((((b - 1) % wide) ^ 1) + 1) % wide, j

    shape = (wide, high)
    far = swap(far, shape, next_chip)
    near = swap(near, shape, own_chip)
    x, f, c, columns = call(
        block_kernel,
        (f32((rows, cols)),) * 3 + (f32((2 * packed, LANE)),),
        [HBM] * 4,
        (VMEM,) * 4,
        [pltpu.VMEM((rows, cols), v.dtype) for v in fields] + [pltpu.SemaphoreType.DMA((4,))],
    )(*fields)
    halo, a, b = call(
        functools.partial(halo_kernel, rows),
        (f32((2 * n, cols)),) + (f32((packed, LANE)),) * 2,
        [VMEM] * 3,
        (VMEM,) * 3,
    )(far, near, columns)
    a = swap(a, shape, even_pair)
    b = swap(b, shape, odd_pair)
    high = (tall, LANE)
    x, r, pair, *strips = call(
        interior_kernel,
        (held((rows, cols)), held((tall, cols)), held((2 * SUB, LANE))) + (held(high),) * 3,
        [VMEM] * 4,
        (VMEM,) * 6,
        [pltpu.VMEM((tall, cols), jnp.float32)] * 2,
    )(x, f, c, halo)
    strip_x, strip_r, pairs = call(
        strip_kernel,
        (held((rows, LANE)), held(high), held((devices, LANE))),
        [VMEM] * 6,
        (VMEM,) * 3,
        [pltpu.VMEM(high, jnp.float32)],
    )(*strips, b, a, pair)
    pairs = lax.all_to_all(pairs, ("bx", "by"), 0, 0, tiled=True)
    x, r, norm = call(
        functools.partial(norm_kernel, rows * cols * devices),
        (f32((rows, cols)), f32((rows, cols)), f32((1,))),
        [VMEM] * 5,
        (HBM,) * 3,
        [pltpu.VMEM((rows, cols), jnp.float32)] * 2 + [pltpu.VMEM((1,), jnp.float32), pltpu.SemaphoreType.DMA((3,))],
    )(pairs, x, r, strip_x, strip_r)
    return (x, r, norm[0])


def solution(mesh):
    spec = P("by", "bx")
    return jax.shard_map(
        per_device, mesh=mesh, in_specs=(spec,) * 4, out_specs=(spec, spec, P()), check_vma=False
    )
```

```python
import functools

import jax
import jax.numpy as jnp
from jax import lax
from jax.experimental import pallas as pl
from jax.experimental.pallas import tpu as pltpu
from jax.sharding import PartitionSpec as P

ITERS = 4
LOW_BOUND = 0.05
HIGH_BOUND = 14.5

SUB = 8
LANE = 128
FIELDS = 3
DEPTH = ITERS + 1
COLUMNS = 2 * SUB
LEFT = LANE // 2 - SUB + DEPTH
VMEM = pl.BlockSpec(memory_space=pltpu.VMEM)
HBM = pl.BlockSpec(memory_space=pltpu.HBM)
GRANT = pltpu.CompilerParams(vmem_limit_bytes=8 << 20)


def call(kernel, shapes, in_specs, out_specs, scratch=(), flops=100000):
    return pl.pallas_call(
        kernel,
        out_shape=shapes,
        in_specs=in_specs,
        out_specs=out_specs,
        scratch_shapes=scratch,
        cost_estimate=pl.CostEstimate(flops=flops, bytes_accessed=0, transcendentals=0),
        compiler_params=GRANT,
    )


def masked_fields(forcing, guess, shift, ocean):
    zero = jnp.zeros_like(forcing)
    sea = ocean > 0
    return (
        jnp.where(sea, guess, zero),
        jnp.where(sea, forcing, zero),
        jnp.where(sea, 6.0 + shift, zero),
    )


def is_odd(axis):
    return lax.rem(lax.axis_index(axis), 2) == 1


def edge_kernel(*refs):
    near_ref, far_ref = refs[4:6]
    low_s, top_s = refs[6:10], refs[10:14]
    sem = refs[14]
    rows = refs[0].shape[0]
    odd = is_odd("by")
    first = pl.multiple_of(jnp.where(odd, 0, rows - SUB), SUB)
    second = pl.multiple_of(jnp.where(odd, rows - SUB, 0), SUB)
    copies = []
    for i in range(4):
        copies.append(pltpu.make_async_copy(refs[i].at[pl.ds(second, SUB), :], top_s[i], sem.at[2 * i + 1]))
        copies.append(pltpu.make_async_copy(refs[i].at[pl.ds(first, SUB), :], low_s[i], sem.at[2 * i]))
    for copy in copies:
        copy.start()
    for copy in copies:
        copy.wait()
    for out, held in ((near_ref, low_s), (far_ref, top_s)):
        for f, field in enumerate(masked_fields(*(ref[...] for ref in held))):
            out[f * SUB : (f + 1) * SUB, :] = field


def place(index):
    per = LANE // COLUMNS
    return index // per * SUB, index % per * COLUMNS


def end_columns(fields, lane, index):
    zero = jnp.zeros((SUB, LANE), jnp.float32)
    left, right = zero, zero
    for f, field in enumerate(fields):
        at = place(index)[1] + f * DEPTH
        first, last = field[:, :LANE], field[:, field.shape[1] - LANE :]
        left = jnp.where((lane >= at) & (lane < at + DEPTH), pltpu.roll(first, at, 1) if at else first, left)
        at = (at + LEFT - DEPTH) % LANE
        here = (lane >= at) & (lane < at + DEPTH) | (lane < at + DEPTH - LANE)
        right = jnp.where(here, pltpu.roll(last, (at + DEPTH) % LANE, 1), right)
    return left, right


def block_kernel(*refs):
    x_ref, r_ref, c_ref, columns_ref = refs[4:8]
    held, sem = refs[8:12], refs[12]
    copies = [pltpu.make_async_copy(refs[i], held[i], sem.at[i]) for i in range(4)]
    for copy in copies:
        copy.start()
    for copy in copies:
        copy.wait()
    fields = masked_fields(*(ref[...] for ref in held))
    for ref, field in zip((x_ref, r_ref, c_ref), fields):
        ref[...] = field
    lane = lax.broadcasted_iota(jnp.int32, (SUB, LANE), 1)
    half = columns_ref.shape[0] // 2
    sums = {}
    for t in range(x_ref.shape[0] // SUB):
        ends = end_columns([field[t * SUB : (t + 1) * SUB] for field in fields], lane, t)
        row = place(t)[0]
        sums[row] = [p + q for p, q in zip(sums[row], ends)] if row in sums else ends
    for row in range(0, half, SUB):
        left, right = sums.get(row, [jnp.zeros((SUB, LANE), jnp.float32)] * 2)
        columns_ref[row : row + SUB, :] = left
        columns_ref[half + row : half + row + SUB, :] = right


def mirrored(tile):
    back = LANE - 1 - lax.broadcasted_iota(jnp.int32, (SUB, LANE), 1)
    up = SUB - 1 - lax.broadcasted_iota(jnp.int32, (SUB, LANE), 0)
    parts = []
    for at in reversed(range(0, tile.shape[1], LANE)):
        part = jnp.take_along_axis(tile[:, at : at + LANE], back, axis=1)
        parts.append(jnp.take_along_axis(part, up, axis=0))
    return jnp.concatenate(parts, axis=1)


def halo_kernel(rows, far_ref, near_ref, columns_ref, halo_ref, a_ref, b_ref):
    odd, odd_x = is_odd("by"), is_odd("bx")
    fold = lax.axis_index("by") == lax.axis_size("by") - 1
    n = FIELDS * SUB
    near, far = near_ref[...], far_ref[...]
    halo_ref[0:n, :] = jnp.where(odd, far, near)
    halo_ref[n : 2 * n, :] = jnp.where(lax.axis_index("by") == 0, 0.0, jnp.where(odd, near, far))

    @pl.when(fold)
    def _():
        for f in range(FIELDS):
            at = slice(f * SUB, (f + 1) * SUB)
            halo_ref[at, :] = mirrored(halo_ref[at, :])

    lane = lax.broadcasted_iota(jnp.int32, (SUB, LANE), 1)
    half = a_ref.shape[0]
    left = [columns_ref[p : p + SUB, :] for p in range(0, half, SUB)]
    right = [columns_ref[half + p : half + p + SUB, :] for p in range(0, half, SUB)]
    for i in range(2):
        fields = [halo_ref[i * n + f * SUB : i * n + (f + 1) * SUB, :] for f in range(FIELDS)]
        first, last = end_columns(fields, lane, rows // SUB + i)
        g = place(rows // SUB + i)[0] // SUB
        left[g], right[g] = left[g] + first, right[g] + last
    for g in range(half // SUB):
        at = slice(g * SUB, (g + 1) * SUB)
        a_ref[at, :] = jnp.where(odd_x, left[g], right[g])
        b_ref[at, :] = jnp.where(odd_x, right[g], left[g])


def coefficients():
    theta = (HIGH_BOUND + LOW_BOUND) / 2.0
    delta = (HIGH_BOUND - LOW_BOUND) / 2.0
    sigma = theta / delta
    rho = 1.0 / sigma
    steps = []
    for _ in range(ITERS):
        following = 1.0 / (2.0 * sigma - rho)
        steps.append((following * rho, 2.0 * following / delta))
        rho = following
    return theta, steps


def pair_add(first, second):
    total = first[0] + second[0]
    backed = total - first[0]
    error = (first[0] - (total - backed)) + (second[0] - backed)
    return (total, (first[1] + second[1]) + error)


def settled(pair):
    upper = pair[0] + pair[1]
    return (upper, pair[1] - (upper - pair[0]))


def pair_tree(pairs):
    while len(pairs) > 1:
        tail = pairs[len(pairs) // 2 * 2 :]
        pairs = [pair_add(pairs[i], pairs[i + 1]) for i in range(0, len(pairs) - 1, 2)] + tail
    return pairs[0]


def pair_total(pairs):
    total = pair_tree(pairs)
    for by in (4, 2, 1):
        total = pair_add(total, tuple(pltpu.roll(v, by, 0) for v in total))
    return total


def sweeps(inner, x_s, d_s, r_s, c_s, weigh):
    tall, wide = d_s.shape
    tiles = tall // SUB
    theta, steps = coefficients()
    row_id = lax.broadcasted_iota(jnp.int32, (SUB, wide), 0)
    first_row, last_row = row_id == 0, row_id == SUB - 1

    def across(i):
        v = d_s[i * SUB : (i + 1) * SUB, :]
        pair = pltpu.roll(v, 1, 1) + pltpu.roll(v, wide - 1, 1)
        mixed = v + 0.5 * pair
        return v, pair, pltpu.roll(mixed, 1, 0), pltpu.roll(mixed, SUB - 1, 0)

    squares = []
    for sweep in range(ITERS + 1):
        head, tail = across(0), across(tiles - 1)
        before, now = tail, head
        for i in range(tiles):
            if i < tiles - 2:
                after = across(i + 1)
            else:
                after = tail if i == tiles - 2 else head
            v, pair, down, up = now
            from_below = jnp.where(first_row, before[2], down)
            from_above = jnp.where(last_row, after[3], up)
            at = slice(i * SUB, (i + 1) * SUB)
            c = c_s[at, :]
            image = jnp.where(c > 0.0, c * v - (pair + (from_below + from_above)), jnp.zeros_like(c))
            r = r_s[at, :] - image
            if sweep < ITERS:
                r_s[at, :] = r
                if sweep == 0:
                    d = r * (1.0 / theta)
                else:
                    keep, gain = steps[sweep - 1]
                    d = keep * v + gain * r
                d_s[at, :] = d
                if i < inner:
                    x_s[at, :] = (v if sweep == 0 else x_s[at, :]) + d
            elif i < inner:
                r_s[at, :] = r
                r = jnp.where(weigh, r, jnp.zeros_like(r))
                squares.append(jnp.sum(r * r, axis=1, keepdims=True))
            before, now = now, after
    zero = jnp.zeros_like(squares[0])
    return pair_total([(q, zero) for q in squares])


def staggered(inner, fill, x_s, r_s, c_s, weigh, lag):
    tall, wide = c_s.shape
    tiles = tall // SUB
    theta, steps = coefficients()
    row_id = lax.broadcasted_iota(jnp.int32, (SUB, wide), 0)
    first_row, last_row = row_id == 0, row_id == SUB - 1
    order = [tiles - 1] + list(range(tiles - 1))

    def across(v):
        pair = pltpu.roll(v, 1, 1) + pltpu.roll(v, wide - 1, 1)
        mixed = v + 0.5 * pair
        return v, pair, pltpu.roll(mixed, 1, 0), pltpu.roll(mixed, SUB - 1, 0)

    squares = []
    held = [{} for _ in range(ITERS + 1)]
    for step in range(tiles + 1 + lag * ITERS):
        if step < tiles:
            held[0][step] = across(fill(order[step]))
        for sweep in range(ITERS + 1):
            p = step - 1 - lag * sweep
            if not 0 <= p < tiles:
                continue
            v, pair, down, up = held[sweep][p]
            before, after = held[sweep].pop(p - 1, None), held[sweep].get(p + 1)
            main = order[p] < inner
            if sweep == ITERS and not main:
                continue
            from_below = down if before is None else jnp.where(first_row, before[2], down)
            from_above = up if after is None else jnp.where(last_row, after[3], up)
            at = slice(order[p] * SUB, (order[p] + 1) * SUB)
            c = c_s[at, :]
            image = jnp.where(c > 0.0, c * v - (pair + (from_below + from_above)), jnp.zeros_like(c))
            r = r_s[at, :] - image
            r_s[at, :] = r
            if sweep < ITERS:
                if sweep == 0:
                    d = r * (1.0 / theta)
                else:
                    keep, gain = steps[sweep - 1]
                    d = keep * v + gain * r
                held[sweep + 1][p] = across(d)
                if main:
                    x_s[at, :] = (v if sweep == 0 else x_s[at, :]) + d
            else:
                r = jnp.where(weigh, r, jnp.zeros_like(r))
                squares.append(jnp.sum(r * r, axis=1, keepdims=True))
    zero = jnp.zeros_like(squares[0])
    return pair_total([(q, zero) for q in squares])


def interior_kernel(x_ref, f_ref, c_ref, halo_ref, out_x_ref, out_r_ref, pair_ref, strip_x, strip_r, strip_c, d_s, c_s):
    rows, cols = x_ref.shape
    high = d_s.shape[0]
    n = FIELDS * SUB
    lane = lax.broadcasted_iota(jnp.int32, (high, LANE), 1)
    left, right = (lane >= LEFT) & (lane < LEFT + 2 * SUB), lane >= LANE - 2 * SUB
    for f, (ref, main, strip) in enumerate(((d_s, x_ref, strip_x), (out_r_ref, f_ref, strip_r), (c_s, c_ref, strip_c))):
        ref[0:rows, :] = main[...]
        ref[rows : rows + SUB, :] = halo_ref[f * SUB : (f + 1) * SUB, :]
        ref[rows + SUB : high, :] = halo_ref[n + f * SUB : n + (f + 1) * SUB, :]
        ends = jnp.where(left, pltpu.roll(ref[:, 0:LANE], LEFT, 1), 0.0)
        strip[...] = jnp.where(right, ref[:, cols - LANE : cols], ends)
    column = lax.broadcasted_iota(jnp.int32, (SUB, cols), 1)
    weigh = (column >= SUB) & (column < cols - SUB)
    upper, lower = sweeps(rows // SUB, out_x_ref, d_s, out_r_ref, c_s, weigh)
    pair_ref[0:SUB, :] = jnp.broadcast_to(upper, (SUB, LANE))
    pair_ref[SUB : 2 * SUB, :] = jnp.broadcast_to(lower, (SUB, LANE))


def strip_kernel(strip_x, strip_r, strip_c, b_ref, a_ref, pair_ref, out_x_ref, out_r_ref, pairs_ref, c_s):
    odd_x = is_odd("bx")
    a, b = a_ref[...], b_ref[...]
    left, right = jnp.where(odd_x, a, b), jnp.where(odd_x, b, a)
    start = LEFT - DEPTH
    lane = lax.broadcasted_iota(jnp.int32, (SUB, LANE), 1)
    ghost = ((lane >= start) & (lane < LEFT)) | (lane < DEPTH)

    def fill(t):
        row, at = place(t)
        rows = slice(t * SUB, (t + 1) * SUB)
        both = jnp.where((lane >= at) & (lane < at + COLUMNS), right[row : row + SUB], left[row : row + SUB])
        values = []
        for f, strip in enumerate((strip_x, strip_r, strip_c)):
            by = (LANE - at - f * DEPTH) % LANE
            values.append(jnp.where(ghost, pltpu.roll(both, by, 1) if by else both, strip[rows, :]))
        out_r_ref[rows, :], c_s[rows, :] = values[1:]
        return values[0]

    lane = lax.broadcasted_iota(jnp.int32, (SUB, LANE), 1)
    weigh = ((lane >= LEFT) & (lane < LEFT + SUB)) | (lane >= LANE - SUB)
    ends = staggered(out_x_ref.shape[0] // SUB, fill, out_x_ref, out_r_ref, c_s, weigh, 3)
    upper, lower = settled(pair_add(ends, (pair_ref[0:SUB, :], pair_ref[SUB : 2 * SUB, :])))
    tile = jnp.where(lane < LANE // 2, upper, lower)
    for i in range(pairs_ref.shape[0] // SUB):
        pairs_ref[i * SUB : (i + 1) * SUB, :] = tile


def norm_kernel(cells, pairs_ref, x_ref, r_ref, strip_x, strip_r, x_hbm, r_hbm, norm_hbm, x_s, r_s, norm_s, sem):
    rows, cols = x_s.shape
    lane = lax.broadcasted_iota(jnp.int32, (rows, LANE), 1)
    copies = []
    for i, (main, strip, joined, out) in enumerate(((x_ref, strip_x, x_s, x_hbm), (r_ref, strip_r, r_s, r_hbm))):
        joined[...] = main[0:rows, :]
        ends = strip[0:rows, :]
        joined[:, 0:LANE] = jnp.where(lane < SUB, pltpu.roll(ends, LANE - LEFT, 1), joined[:, 0:LANE])
        joined[:, cols - LANE : cols] = jnp.where(lane >= LANE - SUB, ends, joined[:, cols - LANE : cols])
        copies.append(pltpu.make_async_copy(joined, out, sem.at[i]))
        copies[i].start()
    pairs = []
    for i in range(pairs_ref.shape[0] // SUB):
        upper = pairs_ref[i * SUB : (i + 1) * SUB, :]
        pairs.append((upper, pltpu.roll(upper, LANE // 2, 1)))
    upper, lower = settled(pair_total(pairs))
    norm_s[...] = jnp.sqrt((upper + lower) * (1.0 / cells))[0, 0:1]
    copies.append(pltpu.make_async_copy(norm_s, norm_hbm, sem.at[2]))
    copies[2].start()
    for copy in copies:
        copy.wait()


def swap(value, mesh_shape, partner):
    wide, high = mesh_shape
    moves = []
    for b in range(wide):
        for j in range(high):
            other = partner(b, j)
            if other is not None:
                moves.append((b * high + j, other[0] * high + other[1]))
    return lax.ppermute(value, ("bx", "by"), moves)


def per_device(forcing, guess, shift, ocean):
    rows, cols = forcing.shape
    wide, high = lax.axis_size("bx"), lax.axis_size("by")
    devices = wide * high
    assert rows % SUB == 0 and cols % LANE == 0 and devices % SUB == 0
    assert wide % 2 == 0 and high % 2 == 0
    assert FIELDS * DEPTH <= COLUMNS
    n = FIELDS * SUB
    tall = rows + 2 * SUB
    packed = -(-tall // (SUB * (LANE // COLUMNS))) * SUB
    f32 = functools.partial(jax.ShapeDtypeStruct, dtype=jnp.float32)
    held = functools.partial(pltpu.VMEM, dtype=jnp.float32)
    fields = [pltpu.with_memory_space_constraint(v, pltpu.HBM) for v in (forcing, guess, shift, ocean)]
    edges = [pltpu.VMEM((SUB, cols), v.dtype) for v in fields]
    near, far = call(
        edge_kernel,
        (f32((n, cols)),) * 2,
        [HBM] * 4,
        (VMEM,) * 2,
        edges * 2 + [pltpu.SemaphoreType.DMA((8,))],
    )(*fields)

    def own_chip(b, j):
        return (b, j ^ 1)

    def next_chip(b, j):
        if j == 0:
            return (wide - 1 - b, j)
        if j == high - 1:
            return (wide - 1 - b, j)
        return (b, ((j - 1) ^ 1) + 1)

    def even_pair(b, j):
        return (b ^ 1, j)

    def odd_pair(b, j):
        return ((((b - 1) % wide) ^ 1) + 1) % wide, j

    shape = (wide, high)
    far = swap(far, shape, next_chip)
    near = swap(near, shape, own_chip)
    x, f, c, columns = call(
        block_kernel,
        (f32((rows, cols)),) * 3 + (f32((2 * packed, LANE)),),
        [HBM] * 4,
        (VMEM,) * 4,
        [pltpu.VMEM((rows, cols), v.dtype) for v in fields] + [pltpu.SemaphoreType.DMA((4,))],
    )(*fields)
    halo, a, b = call(
        functools.partial(halo_kernel, rows),
        (f32((2 * n, cols)),) + (f32((packed, LANE)),) * 2,
        [VMEM] * 3,
        (VMEM,) * 3,
    )(far, near, columns)
    a = swap(a, shape, even_pair)
    b = swap(b, shape, odd_pair)
    high = (tall, LANE)
    x, r, pair, *strips = call(
        interior_kernel,
        (held((rows, cols)), held((tall, cols)), held((2 * SUB, LANE))) + (held(high),) * 3,
        [VMEM] * 4,
        (VMEM,) * 6,
        [pltpu.VMEM((tall, cols), jnp.float32)] * 2,
    )(x, f, c, halo)
    strip_x, strip_r, pairs = call(
        strip_kernel,
        (held((rows, LANE)), held(high), held((devices, LANE))),
        [VMEM] * 6,
        (VMEM,) * 3,
        [pltpu.VMEM(high, jnp.float32)],
    )(*strips, b, a, pair)
    pairs = lax.all_to_all(pairs, ("bx", "by"), 0, 0, tiled=True)
    x, r, norm = call(
        functools.partial(norm_kernel, rows * cols * devices),
        (f32((rows, cols)), f32((rows, cols)), f32((1,))),
        [VMEM] * 5,
        (HBM,) * 3,
        [pltpu.VMEM((rows, cols), jnp.float32)] * 2 + [pltpu.VMEM((1,), jnp.float32), pltpu.SemaphoreType.DMA((3,))],
    )(pairs, x, r, strip_x, strip_r)
    return (x, r, norm[0])


def solution(mesh):
    spec = P("by", "bx")
    return jax.shard_map(
        per_device, mesh=mesh, in_specs=(spec,) * 4, out_specs=(spec, spec, P()), check_vma=False
    )
```
